8 devices in a mesh: data: 2 (over z, y), dap: 4 (over x, core).
Axes of the slice: x: 2, y: 2, z: 1, core: 2. Of those that a mesh axis runs over, the one named last changes fastest.
Arguments:
- msa_act: bfloat16 [4, 128, 128, 256], P('data', 'dap'), parts along dimension 0
- pair_act: bfloat16 [4, 128, 128, 128], P('data', 'dap'), parts along dimension 0
- msa_mask: int32 [4, 128, 128], P('data'), parts along dimension 0
- res_mask: int32 [4, 128], P('data'), parts along dimension 0
- w_row_bias: bfloat16 [128, 8], replicated
- w_row_qkvg: bfloat16 [256, 4, 8, 32], replicated
- w_row_out: bfloat16 [8, 32, 256], replicated
- w_col_qkvg: bfloat16 [256, 4, 8, 32], replicated
- w_col_out: bfloat16 [8, 32, 256], replicated
- w_opm_ac: bfloat16 [256, 2, 32], replicated
- w_opm_out: bfloat16 [32, 32, 128], replicated
- w_ts_bias: bfloat16 [128, 4], replicated
- w_ts_qkvg: bfloat16 [128, 4, 4, 32], replicated
- w_ts_out: bfloat16 [4, 32, 128], replicated
- w_te_bias: bfloat16 [128, 4], replicated
- w_te_qkvg: bfloat16 [128, 4, 4, 32], replicated
- w_te_out: bfloat16 [4, 32, 128], replicated
Outputs:
- output 1: bfloat16 [4, 128, 128, 256], P('data', 'dap'), parts along dimension 0
- output 2: bfloat16 [4, 128, 128, 128], P('data', 'dap'), parts along dimension 0
There are 2 independent parts. The reference program is written for one: setup_inputs(seed, part) draws one part's arguments, and reference() takes and returns one part's arrays. A program takes and returns all parts, laid end to end along the dimension named above; an argument that names none is the same for every part.
All inputs are finite; a program needn't handle non-finite values.
Results may differ from the reference program's by a relative error of at most 0.0153101.
Values are sent between devices in bfloat16 or wider.
A program may use at most 1 GiB of HBM per device.

```python
import jax
import jax.numpy as jnp
from jax import lax

CROPS = 2
NS = 128
NR = 128
C_M = 256
C_Z = 128
MSA_HEADS = 8
MSA_HEAD = 32
TRI_HEADS = 4
TRI_HEAD = 32
OPM_DIM = 32
SCORE_ELEMS = 8388608
MASK_SCALE = 10000.0
LN_EPS = 1e-5
OPM_EPS = 1e-3


def as_float(tensor):
    return tensor.astype(jnp.float32)


def layer_norm(tensor):
    x_float = tensor.astype(jnp.float32)
    mean_val = jnp.mean(x_float, axis=-1, keepdims=True)
    centred = x_float - mean_val
    var_val = jnp.mean(centred * centred, axis=-1, keepdims=True)
    return (centred * lax.rsqrt(var_val + LN_EPS)).astype(jnp.bfloat16)


def mask_to_bias(mask):
    return (mask.astype(jnp.float32) - 1.0) * MASK_SCALE


def rows_per_map(n_rows, per_row):
    return max(1, min(n_rows, SCORE_ELEMS // per_row))


def gated_attention(x_row, key_bias, pair_bias, w_qkvg, w_out):
    normed = layer_norm(x_row)
    proj_all = jnp.einsum('lc,cghd->glhd', as_float(normed), as_float(w_qkvg))
    queries = proj_all[0].astype(jnp.bfloat16)
    keys_bf = proj_all[1].astype(jnp.bfloat16)
    values_bf = proj_all[2].astype(jnp.bfloat16)
    gate_sig = jax.nn.sigmoid(proj_all[3])
    inv_sqrt = queries.shape[-1] ** -0.5
    logits = jnp.einsum('qhd,khd->hqk', as_float(queries), as_float(keys_bf)) * inv_sqrt + key_bias
    if pair_bias is not None:
        logits = logits + as_float(pair_bias)
    attn_prob = jax.nn.softmax(logits, axis=-1).astype(jnp.bfloat16)
    mixed = jnp.einsum('hqk,khd->qhd', as_float(attn_prob), as_float(values_bf)) * gate_sig
    update = jnp.einsum('qhd,hdc->qc', as_float(mixed.astype(jnp.bfloat16)), as_float(w_out))
    return (x_row.astype(jnp.float32) + update).astype(jnp.bfloat16)


def attend_rows(row_stack, key_rows, pair_bias, w_qkvg, w_out):
    n_rows = row_stack.shape[0]
    length = row_stack.shape[1]
    n_heads = w_qkvg.shape[2]
    return lax.map(lambda row_in: gated_attention(row_in[0], row_in[1], pair_bias, w_qkvg, w_out),
                   (row_stack, key_rows), batch_size=rows_per_map(n_rows, n_heads * length * length))


def pair_bias_of(pair_act, w_bias):
    return jnp.einsum('ijc,ch->hij', as_float(layer_norm(pair_act)), as_float(w_bias)).astype(jnp.bfloat16)


def triangle_start(pair_act, res_mask, w_bias, w_qkvg, w_out):
    n_res = pair_act.shape[0]
    key_rows = jnp.broadcast_to(mask_to_bias(res_mask)[None, :], (n_res, n_res))
    return attend_rows(pair_act, key_rows, pair_bias_of(pair_act, w_bias), w_qkvg, w_out)


def outer_product_mean(msa_act, pair_act, msa_mask, w_opm_ac, w_opm_out):
    mask_t = msa_mask.astype(jnp.float32).T
    proj_ac = jnp.einsum('sic,cpe->pise', as_float(layer_norm(msa_act)), as_float(w_opm_ac)).astype(jnp.bfloat16)
    left_proj = as_float(proj_ac[0]) * mask_t[:, :, None]
    right_proj = as_float(proj_ac[1]) * mask_t[:, :, None]
    norm_pairs = jnp.dot(mask_t, mask_t.T)
    n_res = right_proj.shape[0]
    width = right_proj.shape[2]

    def one_row(row_in):
        left_row, norm_row, pair_row = row_in
        outer = jnp.einsum('se,jsf->jef', left_row, right_proj) / (norm_row[:, None, None] + OPM_EPS)
        update = jnp.einsum('jef,efc->jc', as_float(outer.astype(jnp.bfloat16)), as_float(w_opm_out))
        return (pair_row.astype(jnp.float32) + update).astype(jnp.bfloat16)

    return lax.map(one_row, (left_proj, norm_pairs, pair_act), batch_size=rows_per_map(n_res, n_res * width * width))


def evoformer_crop(msa_act, pair_act, msa_mask, res_mask, weights):
    (w_row_bias, w_row_qkvg, w_row_out, w_col_qkvg, w_col_out, w_opm_ac, w_opm_out,
     w_ts_bias, w_ts_qkvg, w_ts_out, w_te_bias, w_te_qkvg, w_te_out) = weights
    msa_act = attend_rows(msa_act, mask_to_bias(msa_mask), pair_bias_of(pair_act, w_row_bias), w_row_qkvg, w_row_out)
    msa_cols = attend_rows(jnp.swapaxes(msa_act, 0, 1), mask_to_bias(msa_mask.T), None, w_col_qkvg, w_col_out)
    msa_act = jnp.swapaxes(msa_cols, 0, 1)
    pair_act = outer_product_mean(msa_act, pair_act, msa_mask, w_opm_ac, w_opm_out)
    pair_act = triangle_start(pair_act, res_mask, w_ts_bias, w_ts_qkvg, w_ts_out)
    pair_cols = triangle_start(jnp.swapaxes(pair_act, 0, 1), res_mask, w_te_bias, w_te_qkvg, w_te_out)
    return msa_act, jnp.swapaxes(pair_cols, 0, 1)


def normal_weight(key, shape, fan_in, gain):
    return (jax.random.normal(key, shape, jnp.float32) * (gain * fan_in ** -0.5)).astype(jnp.bfloat16)


def qkvg_weight(key, width, n_heads, head_dim):
    gains = jnp.array([1.5, 1.5, 1.0, 1.0], jnp.float32)[None, :, None, None]
    draw = jax.random.normal(key, (width, 4, n_heads, head_dim), jnp.float32)
    return (draw * gains * width ** -0.5).astype(jnp.bfloat16)


def setup_inputs(seed: int = 0, part: int = 0) -> dict:
    part_keys = jax.random.split(jax.random.fold_in(jax.random.key(seed), part), 5)
    w_keys = jax.random.split(jax.random.key(seed + 1), 13)
    base = jax.random.normal(part_keys[0], (CROPS, 1, NR, C_M), jnp.float32)
    noise = jax.random.normal(part_keys[1], (CROPS, NS, NR, C_M), jnp.float32)
    msa_act = (0.6 * base + 0.8 * noise).astype(jnp.bfloat16)
    pair_act = jax.random.normal(part_keys[2], (CROPS, NR, NR, C_Z), jnp.float32).astype(jnp.bfloat16)
    msa_mask = (jax.random.randint(part_keys[3], (CROPS, NS, NR), 0, 5) > 0).astype(jnp.int32)
    res_mask = (jax.random.randint(part_keys[4], (CROPS, NR), 0, 4) > 0).astype(jnp.int32)
    msa_width = MSA_HEADS * MSA_HEAD
    tri_width = TRI_HEADS * TRI_HEAD
    return {
        'msa_act': msa_act,
        'pair_act': pair_act,
        'msa_mask': msa_mask,
        'res_mask': res_mask,
        'w_row_bias': normal_weight(w_keys[0], (C_Z, MSA_HEADS), C_Z, 2.0),
        'w_row_qkvg': qkvg_weight(w_keys[1], C_M, MSA_HEADS, MSA_HEAD),
        'w_row_out': normal_weight(w_keys[2], (MSA_HEADS, MSA_HEAD, C_M), msa_width, 1.0),
        'w_col_qkvg': qkvg_weight(w_keys[3], C_M, MSA_HEADS, MSA_HEAD),
        'w_col_out': normal_weight(w_keys[4], (MSA_HEADS, MSA_HEAD, C_M), msa_width, 1.0),
        'w_opm_ac': normal_weight(w_keys[5], (C_M, 2, OPM_DIM), C_M, 1.0),
        'w_opm_out': normal_weight(w_keys[6], (OPM_DIM, OPM_DIM, C_Z), OPM_DIM * OPM_DIM, 1.0),
        'w_ts_bias': normal_weight(w_keys[7], (C_Z, TRI_HEADS), C_Z, 2.0),
        'w_ts_qkvg': qkvg_weight(w_keys[8], C_Z, TRI_HEADS, TRI_HEAD),
        'w_ts_out': normal_weight(w_keys[9], (TRI_HEADS, TRI_HEAD, C_Z), tri_width, 1.0),
        'w_te_bias': normal_weight(w_keys[10], (C_Z, TRI_HEADS), C_Z, 2.0),
        'w_te_qkvg': qkvg_weight(w_keys[11], C_Z, TRI_HEADS, TRI_HEAD),
        'w_te_out': normal_weight(w_keys[12], (TRI_HEADS, TRI_HEAD, C_Z), tri_width, 1.0),
    }


def reference(msa_act, pair_act, msa_mask, res_mask, w_row_bias, w_row_qkvg, w_row_out, w_col_qkvg, w_col_out,
              w_opm_ac, w_opm_out, w_ts_bias, w_ts_qkvg, w_ts_out, w_te_bias, w_te_qkvg, w_te_out):
    weights = (w_row_bias, w_row_qkvg, w_row_out, w_col_qkvg, w_col_out, w_opm_ac, w_opm_out,
               w_ts_bias, w_ts_qkvg, w_ts_out, w_te_bias, w_te_qkvg, w_te_out)
    msa_out, pair_out = lax.map(lambda crop_in: evoformer_crop(crop_in[0], crop_in[1], crop_in[2], crop_in[3], weights),
                                (msa_act, pair_act, msa_mask, res_mask))
    return msa_out, pair_out
```

```python
import functools

import jax
import jax.numpy as jnp
from jax import lax
from jax.experimental import pallas as pl
from jax.experimental.pallas import tpu as pltpu
from jax.sharding import PartitionSpec as P

F32 = jnp.float32
BF16 = jnp.bfloat16
MASK_SCALE = 10000.0
LN_EPS = 1e-5
OPM_EPS = 1e-3
LOG2E = 1.4426950408889634
HEAD_DIM = 32
N = 128
B = 32
W = 256
K1 = 1024
COL_PITCH = 40
TRI_PITCH = 24
SCALE2 = (HEAD_DIM ** -0.5) * LOG2E
PART_AXIS = 'data'
GROUP_AXIS = 'dap'
MESH_ID = pl.DeviceIdType.MESH
NT = (((1,), (1,)), ((), ()))
NN = (((1,), (0,)), ((), ()))
TN = (((0,), (0,)), ((), ()))


def mm(lhs, rhs, dims):
    return lax.dot_general(lhs, rhs, dims, preferred_element_type=F32)


def layer_norm(xf):
    mean = jnp.mean(xf, axis=-1, keepdims=True)
    cen = xf - mean
    var = jnp.mean(cen * cen, axis=-1, keepdims=True)
    return (cen * lax.rsqrt(var + LN_EPS)).astype(BF16)


class Attention:
    def __init__(self, st, wt_ref, wo_ref, n_heads, load_x, bias_of, mask_of, emit, post=None):
        self.qs, self.ks, self.vs, self.gs, self.lg, self.mx, self.os = st
        self.wt, self.wo, self.n_heads, self.hd = wt_ref, wo_ref, n_heads, n_heads * HEAD_DIM
        self.load_x, self.bias_of, self.mask_of, self.emit, self.post = load_x, bias_of, mask_of, emit, post
        self.items = [(u, h) for u in range(2) for h in range(0, n_heads, 2)]

    def p_part(self, y, i, part):
        hd = self.hd
        w = self.wt[part * hd:(part + 1) * hd]
        if part == 0:
            self.qs[i % 2, 0:hd] = mm(w, y, NT).astype(BF16)
        elif part == 1:
            self.ks[i % 2, :, 0:hd] = mm(y, w, NT).astype(BF16)
        elif part == 2:
            self.vs[i % 4, 0:hd] = mm(w, y, NT).astype(BF16)
        else:
            self.gs[i % 4, 0:hd] = jax.nn.sigmoid(mm(w, y, NT))

    def l_part(self, p, i, item):
        u, h = item
        tok = slice(N * u, N * u + N)
        blocks = []
        for hh in (h, h + 1):
            h4 = hh % 4
            rows = [self.qs[i % 2, B * hh:B * hh + B, tok]]
            if h4 > 0:
                rows.insert(0, jnp.zeros((B * h4, N), BF16))
            if h4 < 3:
                rows.append(jnp.zeros((N - B - B * h4, N), BF16))
            blocks.append(jnp.concatenate(rows, axis=0))
        g0 = h // 4 * N
        logits = mm(self.ks[i % 2, tok, g0:g0 + N], jnp.concatenate(blocks, axis=1), NN)
        mask_col = self.mask_of(p, u)
        for n, hh in enumerate((h, h + 1)):
            lg = logits[:, N * n:N * n + N] * SCALE2
            bias = self.bias_of(hh)
            if bias is not None:
                lg = lg + bias
            if mask_col is not None:
                lg = lg + mask_col
            row = u * self.n_heads + hh
            self.lg[i % 2, row] = lg
            self.mx[i % 2, row:row + 1] = jnp.max(lg, axis=0, keepdims=True)

    def s_part(self, i, item):
        u, h = item
        tok = slice(N * u, N * u + N)
        ps, inv = [], []
        for hh in (h, h + 1):
            row = u * self.n_heads + hh
            ex = jnp.exp2(self.lg[i % 2, row] - self.mx[i % 2, row:row + 1])
            inv.append(1.0 / jnp.sum(ex, axis=0, keepdims=True))
            ps.append(ex.astype(BF16))
        h0 = h * B
        ov = mm(self.vs[i % 4, h0:h0 + 2 * B, tok], jnp.concatenate(ps, axis=1), NN)
        o = jnp.concatenate([ov[0:B, 0:N] * inv[0], ov[B:2 * B, N:W] * inv[1]], axis=0)
        self.os[i % 2, h0:h0 + 2 * B, tok] = (o * self.gs[i % 4, h0:h0 + 2 * B, tok]).astype(BF16)

    def o_part(self, p, i):
        self.emit(p, i % 2, self.load_x(p) + mm(self.os[i % 2, 0:self.hd], self.wo[...], TN))

    def step(self, p, i, last):
        if self.post is not None:
            self.post(jnp.maximum(p - 2, 0), i % 2)
        self.o_part(jnp.maximum(p - 1, 0), i - 1)
        y = layer_norm(self.load_x(jnp.minimum(p + 2, last)))
        nxt = jnp.minimum(p + 1, last)
        for n, item in enumerate(self.items):
            self.l_part(nxt, i + 1, item)
            self.s_part(i, item)
            for part in range(4):
                if part * len(self.items) // 4 == n:
                    self.p_part(y, i + 2, part)

    def begin(self):
        for i in range(2):
            y = layer_norm(self.load_x(i))
            for part in range(4):
                self.p_part(y, i, part)
        for item in self.items:
            self.l_part(0, 0, item)

    def end(self, last):
        self.o_part(last, 3)
        if self.post is not None:
            self.post(last - 1, 0)
            self.post(last, 1)


def rows_at(start, size):
    return pl.ds(pl.multiple_of(start, size), size)


def side_by_side(b):
    return jnp.concatenate([b[:, :N], b[:, N:]], axis=0)


def mega(m_in, z_in, mask_ref, mrow_ref, mcol_ref, mres_ref, w_rb, w_tsb, w_teb, w_row, w_row_o, w_col, w_col_o, w_ac, w_oo,
         w_ts, w_ts_o, w_te, w_te_o, m_out, z_out,
         zr, zot, ms, xx, rs, bb, bbf, bt, xf0, xf1, of0, of1, mo, at, ctx, ctf, cp, ninv, mtr, woot, rr,
         bs, bts, be, bte, zx, zs, zf, zof, zo, qs, ks, vs, gs, lgs, mxs, ots, nw, wtsb, wteb,
         l_sem, mi_s, mi_r, zi_s, zi_r, b_s, b_r, x_s, x_r, mo_s, mo_r, mo_l, c_s, c_r, bs_s, bs_r, be_s, be_r,
         zx_s, zx_r, zo_s, zo_r, zo_l):
    st = (qs, ks, vs, gs, lgs, mxs, ots)
    dat = lax.axis_index(PART_AXIS)
    dev = lax.axis_index(GROUP_AXIS)
    x = dev // 2
    c = dev % 2
    ox = 1 - x

    def peer(flip):
        px = ox if flip >= 2 else x
        pc = (1 - c) if flip % 2 else c
        return px * 2 + pc

    def remote(src, dst, s_sem, r_sem, flip):
        return pltpu.make_async_remote_copy(src, dst, s_sem, r_sem, device_id=(dat, peer(flip)),
                                            device_id_type=MESH_ID)

    barrier = pltpu.get_barrier_semaphore()
    for flip in (1, 2, 3):
        pl.semaphore_signal(barrier, inc=1, device_id=(dat, peer(flip)), device_id_type=MESH_ID)
    cp_zo = pltpu.make_async_copy(z_in.at[ox], zot, l_sem.at[0])
    cp_zr = pltpu.make_async_copy(z_in.at[x], zr.at[x], l_sem.at[1])
    cp_m = pltpu.make_async_copy(m_in.at[x], ms.at[x], l_sem.at[2])
    cp_zo.start()
    cp_zr.start()
    cp_m.start()
    pl.semaphore_wait(barrier, 3)

    def m_chunk(j):
        return remote(m_in.at[ox, pl.ds(4 * j, 4)], ms.at[x, pl.ds(4 * j, 4)], mi_s.at[j], mi_r.at[j], 2)

    m_chunk(0).start()

    def bias_rows(load, base):
        def body(g, carry):
            for p in range(4):
                y = layer_norm(load(8 * g + 2 * p).reshape(W, N).astype(F32))
                b = side_by_side(mm(w_rb[...], y, NT)).astype(BF16)
                bb[rows_at(base + 64 * g + 16 * p, 16)] = b
            return carry
        lax.fori_loop(0, 4, body, 0)

    row0 = pl.multiple_of(dev * W, W)
    spare = K1
    cp_zo.wait()
    bias_rows(lambda r: zot[pl.ds(r, 2)], spare)
    b_copies = []
    for n, flip in enumerate((2, 3)):
        b_copies.append(remote(bb.at[pl.ds(spare, W)], bb.at[pl.ds(row0, W)], b_s.at[n], b_r.at[n], flip))
    for cpy in b_copies:
        cpy.start()
    for j in range(1, 8):
        m_chunk(j).start()
    z_copy = remote(z_in.at[ox], zr.at[x], zi_s.at[0], zi_r.at[0], 2)
    z_copy.start()
    cp_zr.wait()

    bias_rows(lambda r: zr[x, pl.ds(r, 2)], row0)
    b_own = remote(bb.at[pl.ds(row0, W)], bb.at[pl.ds(row0, W)], b_s.at[2], b_r.at[2], 1)
    b_own.start()
    b_copies.append(b_own)

    for wdst, wsrc in ((wtsb, w_tsb), (wteb, w_teb)):
        wdst[0:4] = wsrc[...].astype(F32)
        wdst[4:8] = jnp.zeros((4, N), F32)
    mk = mask_ref[x].astype(F32)
    mkb = mk.astype(BF16)
    ninv[...] = 1.0 / (mm(mkb, mkb, TN) + OPM_EPS)
    mtr[...] = jnp.transpose(mk)
    for e in range(B):
        ctf[pl.ds(e * COL_PITCH, B)] = w_oo[B * e:B * e + B].astype(F32)
    def perm_oo(f, carry):
        xf0[rows_at(B * f, B)] = ctf[pl.ds(f, B, stride=COL_PITCH), :]
        return carry
    lax.fori_loop(0, B, perm_oo, 0)
    for t in range(8):
        woot[:, N * t:N * t + N] = jnp.transpose(xf0[N * t:N * t + N, :]).astype(BF16)

    for cpy in b_copies:
        cpy.wait_recv()
    bbf[...] = bb[0:K1].astype(F32) * LOG2E
    for h in range(8):
        bt[h] = jnp.transpose(bbf[pl.ds(h, N, stride=8), :])

    cp_m.wait()

    def x_chunk(ch):
        k = jnp.where(ch < 4, x, ox)
        rows = rows_at(k * B + (ch % 4) * 8, 8)
        return remote(rs.at[rows], xx.at[c, rows], x_s.at[ch], x_r.at[ch], 1)

    def row_seq(p):
        return jnp.where(p < 16, x, ox) * B + 2 * (p % 16)

    def row_x(p):
        s = row_seq(p)
        return ms[s // B, pl.ds(s % B, 2)].reshape(W, W).astype(F32)

    def lane_mask(ref, row, u):
        return jnp.broadcast_to(ref[row][:, u:u + 1], (N, N))

    def row_emit(p, slot, new):
        s = row_seq(p)
        new = new.reshape(2, 2, 2, B, W)
        even, odd = new[:, :, 0], new[:, :, 1]
        xx[c, pl.ds(s, 2)] = jnp.where(c == 0, even, odd).astype(BF16)
        rs[pl.ds(s, 2)] = jnp.where(c == 0, odd, even).astype(BF16)

    row = Attention(st, w_row, w_row_o, 8, row_x, lambda h: bt[h],
                    lambda p, u: lane_mask(mrow_ref, row_seq(p) // 2, u), row_emit)

    def row_four(t, carry):
        @pl.when(jnp.logical_and(t >= 3, t < 7))
        def _():
            m_chunk(2 * t - 6).wait_recv()
            m_chunk(2 * t - 5).wait_recv()

        for e in range(4):
            row.step(4 * t + e, e, 31)

        @pl.when(t > 0)
        def _():
            x_chunk(t - 1).start()
        return carry
    row.begin()
    lax.fori_loop(0, 8, row_four, 0)
    row.end(31)
    x_chunk(7).start()

    def x_wait(ch, carry):
        x_chunk(ch).wait_recv()
        return carry
    lax.fori_loop(0, 8, x_wait, 0)

    def mo_copies(q):
        out = []
        res0 = pl.multiple_of((2 * q + c) * B, B)
        for flip in range(4):
            src = mo.at[pl.ds(peer(flip) * B, B), q]
            dst = m_out.at[x, :, pl.ds(res0, B)]
            if flip == 0:
                out.append(pltpu.make_async_copy(src, dst, mo_l.at[q]))
            else:
                out.append(remote(src, dst, mo_s.at[q, flip - 1], mo_r.at[q, flip - 1], flip))
        return out

    def c_copy(q):
        rows = rows_at((2 * q + c) * K1, K1)
        return remote(ctx.at[rows], ctx.at[rows], c_s.at[q], c_r.at[q], 1)

    def col_x(p):
        return jnp.concatenate([
            jnp.concatenate([ref[pl.ds(2 * p + u, N, stride=COL_PITCH), :] for ref in (xf0, xf1)], axis=1)
            for u in range(2)], axis=0)

    def col_chunk(q, carry):
        for c2 in range(2):
            for k in range(2):
                for r in range(B):
                    v = xx[c2, k * B + r, q].astype(F32)
                    rows = pl.ds(((2 * k + c2) * B + r) * COL_PITCH, B)
                    xf0[rows] = v[:, :N]
                    xf1[rows] = v[:, N:]

        def col_post(p, slot):
            ac = mm(w_ac[...], layer_norm(nw[slot].astype(F32)), NT).astype(BF16).astype(F32)
            for u in range(2):
                loc = q * B + 2 * p + u
                nat = (2 * q + c) * B + 2 * p + u
                acm = (ac[:, N * u:N * u + N] * mtr[pl.ds(nat, 1), :]).astype(BF16)
                at[rows_at(loc * B, B)] = acm[0:B]
                ctx[rows_at(nat * B, B)] = acm[B:2 * B]

        def col_emit(p, slot, new):
            nw[slot] = new.astype(BF16)
            for u in range(2):
                of0[pl.ds(2 * p + u, N, stride=COL_PITCH), :] = new[N * u:N * u + N, :N]
                of1[pl.ds(2 * p + u, N, stride=COL_PITCH), :] = new[N * u:N * u + N, N:]

        col = Attention(st, w_col, w_col_o, 8, col_x, lambda h: None,
                        lambda p, u: lane_mask(mcol_ref, q * 16 + p, u), col_emit, col_post)

        def col_four(t, carry2):
            for e in range(4):
                col.step(4 * t + e, e, 15)
            return carry2
        col.begin()
        lax.fori_loop(0, 4, col_four, 0)
        col.end(15)
        for r in range(N):
            rows = pl.ds(r * COL_PITCH, B)
            mo[r, q] = jnp.concatenate([of0[rows, :], of1[rows, :]], axis=1).astype(BF16)
        c_copy(q).start()
        for cpy in mo_copies(q):
            cpy.start()
        return carry
    lax.fori_loop(0, 2, col_chunk, 0)

    for q in range(2):
        c_copy(q).wait_recv()
    for j in range(N):
        ctf[pl.ds(j * COL_PITCH, B)] = ctx[B * j:B * j + B].astype(F32)

    def perm_c(f, carry):
        cp[rows_at(f * N, N)] = ctf[pl.ds(f, N, stride=COL_PITCH), :].astype(BF16)
        return carry
    lax.fori_loop(0, B, perm_c, 0)
    z_copy.wait_recv()

    def opm_place(ib):
        k, r0 = ib // 4, (ib % 4) * 8
        return k, r0, (2 * k + c) * B + r0

    def opm_outer(ib, slot, fp):
        nat0 = opm_place(ib)[2]
        o = mm(at[rows_at(ib * W, W)], cp[fp * W:fp * W + W], NT)
        for i in range(8):
            nrow = ninv[pl.ds(nat0 + i, 1), :]
            for ff in range(2):
                blk = o[B * i:B * i + B, N * ff:N * ff + N] * nrow
                rr[slot, i, fp * 64 + B * ff:fp * 64 + B * ff + B] = blk.astype(BF16)

    def opm_load(ib, ip):
        k, r0, _ = opm_place(ib)
        return zr[k, pl.ds(r0 + 2 * ip, 2)].reshape(W, N).astype(F32)

    def opm_update(z_old, slot, ip):
        upd_t = mm(woot[...], jnp.concatenate([rr[slot, 2 * ip], rr[slot, 2 * ip + 1]], axis=1), NN)
        zn = (z_old + jnp.concatenate([jnp.transpose(upd_t[:, :N]), jnp.transpose(upd_t[:, N:])], axis=0)).astype(BF16)
        b = side_by_side(mm(wtsb[...].astype(BF16), layer_norm(zn.astype(F32)), NT)).astype(BF16).astype(F32)
        return zn, b

    def opm_store(ib, ip, zn, b):
        k, r0, nat0 = opm_place(ib)
        zr[k, pl.ds(r0 + 2 * ip, 2)] = zn.reshape(2, N, N)
        bs[rows_at((nat0 + 2 * ip) * 8, 16)] = b

    def opm_two(t, carry):
        for e in range(2):
            ib = 2 * t + e
            nxt = jnp.minimum(ib + 1, 7)
            olds = [opm_load(ib, ip) for ip in range(4)]
            news = []
            for ip in range(4):
                for fp in range(4):
                    opm_outer(nxt, 1 - e, ip * 4 + fp)
                news.append(opm_update(olds[ip], e, ip))
            for ip in range(4):
                opm_store(ib, ip, *news[ip])
        return carry
    for fp in range(16):
        opm_outer(0, 0, fp)
    lax.fori_loop(0, 4, opm_two, 0)

    def tri_bias_copies(ref, s_sem, r_sem):
        out = []
        for k in range(2):
            rows = rows_at((2 * k + c) * W, W)
            out.append(remote(ref.at[rows], ref.at[rows], s_sem.at[k], r_sem.at[k], 1))
        return out
    bs_copies = tri_bias_copies(bs, bs_s, bs_r)
    for cpy in bs_copies:
        cpy.start()
    for cpy in bs_copies:
        cpy.wait_recv()
    mres = jnp.broadcast_to(mres_ref[...], (N, N))
    for h in range(4):
        bts[h] = jnp.transpose(bs[pl.ds(h, N, stride=8), :]) * LOG2E + mres

    def zx_copy(ob):
        rows = rows_at(ob * 8, 8)
        return remote(zs.at[rows], zx.at[c, rows], zx_s.at[ob], zx_r.at[ob], 1)

    def ts_x(p):
        return zr[p // 16, pl.ds(2 * (p % 16), 2)].reshape(W, N).astype(F32)

    def ts_post(p, slot):
        b = mm(wteb[...].astype(BF16), layer_norm(nw[slot, :, 0:N].astype(F32)), NT)
        nat = (2 * (p // 16) + c) * B + 2 * (p % 16)
        be[rows_at(nat * 8, 16)] = side_by_side(b).astype(BF16).astype(F32)

    def ts_emit(p, slot, new):
        nw[slot, :, 0:N] = new.astype(BF16)
        new = new.reshape(2, 2, 2, B, N)
        even, odd = new[:, :, 0], new[:, :, 1]
        zx[c, pl.ds(2 * p, 2)] = jnp.where(c == 0, even, odd).astype(BF16)
        zs[pl.ds(2 * p, 2)] = jnp.where(c == 0, odd, even).astype(BF16)

    ts = Attention(st, w_ts, w_ts_o, 4, ts_x, lambda h: bts[h], lambda p, u: None, ts_emit, ts_post)

    def ts_four(ob, carry):
        for e in range(4):
            ts.step(4 * ob + e, e, 31)

        @pl.when(ob > 0)
        def _():
            zx_copy(ob - 1).start()
        return carry
    ts.begin()
    lax.fori_loop(0, 8, ts_four, 0)
    ts.end(31)
    zx_copy(7).start()
    be_copies = tri_bias_copies(be, be_s, be_r)
    for cpy in be_copies:
        cpy.start()
    for cpy in be_copies:
        cpy.wait_recv()
    for h in range(4):
        bte[h] = be[pl.ds(h, N, stride=8), :] * LOG2E + mres

    def zx_wait(ob, carry):
        zx_copy(ob).wait_recv()
        return carry
    lax.fori_loop(0, 8, zx_wait, 0)

    def zo_copies(ci, q, hf):
        out = []
        col0 = pl.multiple_of((2 * q + c) * B + hf * 16, 16)
        h16 = pl.multiple_of(hf * 16, 16)
        for flip in range(4):
            home = peer(flip)
            src = zo.at[pl.ds(home * B, B), q, pl.ds(h16, 16)]
            dst = z_out.at[x, :, pl.ds(col0, 16)]
            if flip == 0:
                out.append(pltpu.make_async_copy(src, dst, zo_l.at[ci]))
            else:
                out.append(remote(src, dst, zo_s.at[ci, flip - 1], zo_r.at[ci, flip - 1], flip))
        return out

    def te_chunk(ci, carry):
        q = ci // 2
        hf = ci % 2
        h16 = pl.multiple_of(hf * 16, 16)
        for c2 in range(2):
            for k in range(2):
                for r in range(B):
                    rows = pl.ds(((2 * k + c2) * B + r) * TRI_PITCH, 16)
                    zf[rows] = zx[c2, k * B + r, q, pl.ds(h16, 16), :].astype(F32)

        def te_x(p):
            return jnp.concatenate([zf[pl.ds(2 * p + u, N, stride=TRI_PITCH), :] for u in range(2)], axis=0)

        def te_emit(p, slot, new):
            for u in range(2):
                zof[pl.ds(2 * p + u, N, stride=TRI_PITCH), :] = new[N * u:N * u + N]

        te = Attention(st, w_te, w_te_o, 4, te_x, lambda h: bte[h], lambda p, u: None, te_emit)

        def te_four(t, carry2):
            for e in range(4):
                te.step(4 * t + e, e, 7)
            return carry2
        te.begin()
        lax.fori_loop(0, 2, te_four, 0)
        te.end(7)
        for r in range(N):
            zo[r, q, pl.ds(h16, 16), :] = zof[pl.ds(r * TRI_PITCH, 16), :].astype(BF16)
        for cpy in zo_copies(ci, q, hf):
            cpy.start()
        return carry
    lax.fori_loop(0, 4, te_chunk, 0)

    for cpy in b_copies + bs_copies + be_copies + [z_copy]:
        cpy.wait_send()
    def drain8(j, carry):
        m_chunk(j).wait_send()
        zx_copy(j).wait_send()
        x_chunk(j).wait_send()
        return carry
    lax.fori_loop(0, 8, drain8, 0)
    for q in range(2):
        c_copy(q).wait_send()
        for cpy in mo_copies(q):
            cpy.wait()
    def drain4(ci, carry):
        for cpy in zo_copies(ci, ci // 2, ci % 2):
            cpy.wait()
        return carry
    lax.fori_loop(0, 4, drain4, 0)


def weight_t(w):
    return w.reshape(w.shape[0], -1).T


def solution(mesh):
    rows_spec = P(PART_AXIS, GROUP_AXIS, None, None)
    in_specs = (rows_spec, rows_spec, P(PART_AXIS, None, None), P(PART_AXIS, None)) + (P(),) * 13

    def block(m, z, mask, res_mask, *weights):
        (w_row_bias, w_row_qkvg, w_row_out, w_col_qkvg, w_col_out, w_opm_ac, w_opm_out,
         w_ts_bias, w_ts_qkvg, w_ts_out, w_te_bias, w_te_qkvg, w_te_out) = weights
        dev = lax.axis_index(GROUP_AXIS)
        x = dev // 2
        c = dev % 2
        mbias = (lax.dynamic_index_in_dim(mask, x, 0, False).astype(F32) - 1.0) * (MASK_SCALE * LOG2E)
        mrow = lax.dynamic_index_in_dim(mbias.reshape(2, 2, B, N), c, 1, False)
        mrow = mrow.reshape(B, 2, N).swapaxes(1, 2)
        mcol = lax.dynamic_index_in_dim(mbias.T.reshape(2, 2, B, N), c, 1, False)
        mcol = mcol.reshape(B, 2, N).swapaxes(1, 2)
        mres = (lax.dynamic_index_in_dim(res_mask, x, 0, False).astype(F32) - 1.0) * (MASK_SCALE * LOG2E)
        args = (m, z, mask, mrow, mcol, mres[:, None], w_row_bias.T, w_ts_bias.T, w_te_bias.T,
                weight_t(w_row_qkvg), w_row_out.reshape(W, W), weight_t(w_col_qkvg), w_col_out.reshape(W, W),
                weight_t(w_opm_ac), w_opm_out.reshape(K1, N),
                weight_t(w_ts_qkvg), w_ts_out.reshape(N, N), weight_t(w_te_qkvg), w_te_out.reshape(N, N))
        vm = pl.BlockSpec(memory_space=pltpu.VMEM)
        hbm = pl.BlockSpec(memory_space=pl.ANY)
        V = pltpu.VMEM
        row_z, row_m, sq = (B, N, N), (B, N, W), (N, N)
        scratch = [V(shape, BF16) for shape in (
            (2,) + row_z, row_z, (2,) + row_m, (2, 64, 2, B, W), (64, 2, B, W), (1280, N))]
        scratch += [V(shape, F32) for shape in (
            (K1, N), (8,) + sq) + ((N * COL_PITCH, N),) * 4]
        scratch += [V((N, 2, B, W), BF16), V((2048, N), BF16), V((B * N, N), BF16), V((N * COL_PITCH, N), F32),
                    V((B * N, N), BF16), V(sq, F32), V(sq, F32), V((N, K1), BF16), V((2, 8, K1, N), BF16)]
        scratch += [V(shape, F32) for shape in ((K1, N), (4,) + sq, (K1, N), (4,) + sq)]
        scratch += [V((2, 64, 2, B, N), BF16), V((64, 2, B, N), BF16), V((N * TRI_PITCH, N), F32), V((N * TRI_PITCH, N), F32),
                    V((N, 2, B, N), BF16)]
        scratch += [V((2, W, W), BF16)] * 2 + [V((4, W, W), BF16), V((4, W, W), F32), V((2, 16) + sq, F32),
                    V((2, 16, N), F32), V((2, W, W), BF16), V((2, W, W), BF16), V((8, N), F32), V((8, N), F32)]
        S = pltpu.SemaphoreType.DMA
        scratch += [S(shape) for shape in (
            (3,), (8,), (8,), (1,), (1,), (3,), (3,), (8,), (8,), (2, 3), (2, 3), (2,), (2,), (2,),
            (2,), (2,), (2,), (2,), (8,), (8,), (4, 3), (4, 3), (4,))]
        return pl.pallas_call(
            mega,
            out_shape=(jax.ShapeDtypeStruct(m.shape, BF16), jax.ShapeDtypeStruct(z.shape, BF16)),
            in_specs=[hbm, hbm] + [vm] * 17,
            out_specs=(hbm, hbm),
            scratch_shapes=scratch,
            compiler_params=pltpu.CompilerParams(collective_id=0, has_side_effects=True,
                                                 vmem_limit_bytes=62 << 20),
            name='evoformer_block',
        )(*args)

    return jax.shard_map(block, mesh=mesh, in_specs=in_specs, out_specs=(rows_spec, rows_spec), check_vma=False)
```

```python
import functools

import jax
import jax.numpy as jnp
from jax import lax
from jax.experimental import pallas as pl
from jax.experimental.pallas import tpu as pltpu
from jax.sharding import PartitionSpec as P

F32 = jnp.float32
BF16 = jnp.bfloat16
MASK_SCALE = 10000.0
LN_EPS = 1e-5
OPM_EPS = 1e-3
LOG2E = 1.4426950408889634
HEAD_DIM = 32
N = 128
B = 32
W = 256
K1 = 1024
COL_PITCH = 40
TRI_PITCH = 24
SCALE2 = (HEAD_DIM ** -0.5) * LOG2E
PART_AXIS = 'data'
GROUP_AXIS = 'dap'
MESH_ID = pl.DeviceIdType.MESH
NT = (((1,), (1,)), ((), ()))
NN = (((1,), (0,)), ((), ()))
TN = (((0,), (0,)), ((), ()))


def mm(lhs, rhs, dims):
    return lax.dot_general(lhs, rhs, dims, preferred_element_type=F32)


def layer_norm(xf):
    mean = jnp.mean(xf, axis=-1, keepdims=True)
    cen = xf - mean
    var = jnp.mean(cen * cen, axis=-1, keepdims=True)
    return (cen * lax.rsqrt(var + LN_EPS)).astype(BF16)


class Attention:
    def __init__(self, st, wt_ref, wo_ref, n_heads, load_x, bias_of, mask_of, emit, post=None):
        self.qs, self.ks, self.vs, self.gs, self.lg, self.mx, self.os = st
        self.wt, self.wo, self.n_heads, self.hd = wt_ref, wo_ref, n_heads, n_heads * HEAD_DIM
        self.load_x, self.bias_of, self.mask_of, self.emit, self.post = load_x, bias_of, mask_of, emit, post
        self.items = [(u, h) for u in range(2) for h in range(0, n_heads, 2)]

    def p_part(self, y, i, part):
        hd = self.hd
        w = self.wt[part * hd:(part + 1) * hd]
        if part == 0:
            self.qs[i % 2, 0:hd] = mm(w, y, NT).astype(BF16)
        elif part == 1:
            self.ks[i % 2, :, 0:hd] = mm(y, w, NT).astype(BF16)
        elif part == 2:
            self.vs[i % 4, 0:hd] = mm(w, y, NT).astype(BF16)
        else:
            self.gs[i % 4, 0:hd] = jax.nn.sigmoid(mm(w, y, NT))

    def l_part(self, p, i, item):
        u, h = item
        tok = slice(N * u, N * u + N)
        blocks = []
        for hh in (h, h + 1):
            h4 = hh % 4
            rows = [self.qs[i % 2, B * hh:B * hh + B, tok]]
            if h4 > 0:
                rows.insert(0, jnp.zeros((B * h4, N), BF16))
            if h4 < 3:
                rows.append(jnp.zeros((N - B - B * h4, N), BF16))
            blocks.append(jnp.concatenate(rows, axis=0))
        g0 = h // 4 * N
        logits = mm(self.ks[i % 2, tok, g0:g0 + N], jnp.concatenate(blocks, axis=1), NN)
        mask_col = self.mask_of(p, u)
        for n, hh in enumerate((h, h + 1)):
            lg = logits[:, N * n:N * n + N] * SCALE2
            bias = self.bias_of(hh)
            if bias is not None:
                lg = lg + bias
            if mask_col is not None:
                lg = lg + mask_col
            row = u * self.n_heads + hh
            self.lg[i % 2, row] = lg
            self.mx[i % 2, row:row + 1] = jnp.max(lg, axis=0, keepdims=True)

    def s_part(self, i, item):
        u, h = item
        tok = slice(N * u, N * u + N)
        ps, inv = [], []
        for hh in (h, h + 1):
            row = u * self.n_heads + hh
            ex = jnp.exp2(self.lg[i % 2, row] - self.mx[i % 2, row:row + 1])
            inv.append(1.0 / jnp.sum(ex, axis=0, keepdims=True))
            ps.append(ex.astype(BF16))
        h0 = h * B
        ov = mm(self.vs[i % 4, h0:h0 + 2 * B, tok], jnp.concatenate(ps, axis=1), NN)
        o = jnp.concatenate([ov[0:B, 0:N] * inv[0], ov[B:2 * B, N:W] * inv[1]], axis=0)
        self.os[i % 2, h0:h0 + 2 * B, tok] = (o * self.gs[i % 4, h0:h0 + 2 * B, tok]).astype(BF16)

    def o_part(self, p, i):
        self.emit(p, i % 2, self.load_x(p) + mm(self.os[i % 2, 0:self.hd], self.wo[...], TN))

    def step(self, p, i, last):
        if self.post is not None:
            self.post(jnp.maximum(p - 2, 0), i % 2)
        self.o_part(jnp.maximum(p - 1, 0), i - 1)
        y = layer_norm(self.load_x(jnp.minimum(p + 2, last)))
        nxt = jnp.minimum(p + 1, last)
        for n, item in enumerate(self.items):
            self.l_part(nxt, i + 1, item)
            self.s_part(i, item)
            for part in range(4):
                if part * len(self.items) // 4 == n:
                    self.p_part(y, i + 2, part)

    def begin(self):
        for i in range(2):
            y = layer_norm(self.load_x(i))
            for part in range(4):
                self.p_part(y, i, part)
        for item in self.items:
            self.l_part(0, 0, item)

    def end(self, last):
        self.o_part(last, 3)
        if self.post is not None:
            self.post(last - 1, 0)
            self.post(last, 1)


def rows_at(start, size):
    return pl.ds(pl.multiple_of(start, size), size)


def side_by_side(b):
    return jnp.concatenate([b[:, :N], b[:, N:]], axis=0)


def mega(m_in, z_in, mask_ref, res_ref, w_rb, w_tsb, w_teb, w_row, w_row_o, w_col, w_col_o, w_ac, w_oo,
         w_ts, w_ts_o, w_te, w_te_o, m_out, z_out,
         zr, zot, ms, xx, rs, bb, bbf, bt, xf0, xf1, of0, of1, mo, at, ctx, ctf, cp, ninv, mtr, woot, rr,
         bs, bts, be, bte, zx, zs, zf, zof, zo, qs, ks, vs, gs, lgs, mxs, ots, nw, wtsb, wteb, mcb, mrb, mrs, mrow, mcol, ut,
         l_sem, mi_s, mi_r, zi_s, zi_r, b_s, b_r, x_s, x_r, mo_s, mo_r, mo_l, c_s, c_r, bs_s, bs_r, be_s, be_r,
         zx_s, zx_r, zo_s, zo_r, zo_l):
    st = (qs, ks, vs, gs, lgs, mxs, ots)
    dat = lax.axis_index(PART_AXIS)
    dev = lax.axis_index(GROUP_AXIS)
    x = dev // 2
    c = dev % 2
    ox = 1 - x

    def peer(flip):
        px = ox if flip >= 2 else x
        pc = (1 - c) if flip % 2 else c
        return px * 2 + pc

    def remote(src, dst, s_sem, r_sem, flip):
        return pltpu.make_async_remote_copy(src, dst, s_sem, r_sem, device_id=(dat, peer(flip)),
                                            device_id_type=MESH_ID)

    barrier = pltpu.get_barrier_semaphore()
    for flip in (1, 2, 3):
        pl.semaphore_signal(barrier, inc=1, device_id=(dat, peer(flip)), device_id_type=MESH_ID)
    cp_zo = pltpu.make_async_copy(z_in.at[ox], zot, l_sem.at[0])
    cp_zr = pltpu.make_async_copy(z_in.at[x], zr.at[x], l_sem.at[1])
    cp_m = pltpu.make_async_copy(m_in.at[x], ms.at[x], l_sem.at[2])
    cp_zo.start()
    cp_zr.start()
    cp_m.start()
    pl.semaphore_wait(barrier, 3)

    def m_chunk(j):
        return remote(m_in.at[ox, pl.ds(4 * j, 4)], ms.at[x, pl.ds(4 * j, 4)], mi_s.at[j], mi_r.at[j], 2)

    m_chunk(0).start()

    def bias_rows(load, base):
        def body(g, carry):
            for p in range(4):
                y = layer_norm(load(8 * g + 2 * p).reshape(W, N).astype(F32))
                b = side_by_side(mm(w_rb[...], y, NT)).astype(BF16)
                bb[rows_at(base + 64 * g + 16 * p, 16)] = b
            return carry
        lax.fori_loop(0, 4, body, 0)

    row0 = pl.multiple_of(dev * W, W)
    spare = K1
    cp_zo.wait()
    bias_rows(lambda r: zot[pl.ds(r, 2)], spare)
    b_copies = []
    for n, flip in enumerate((2, 3)):
        b_copies.append(remote(bb.at[pl.ds(spare, W)], bb.at[pl.ds(row0, W)], b_s.at[n], b_r.at[n], flip))
    for cpy in b_copies:
        cpy.start()
    for j in range(1, 8):
        m_chunk(j).start()
    z_copy = remote(z_in.at[ox], zr.at[x], zi_s.at[0], zi_r.at[0], 2)
    z_copy.start()
    cp_zr.wait()

    bias_rows(lambda r: zr[x, pl.ds(r, 2)], row0)
    b_own = remote(bb.at[pl.ds(row0, W)], bb.at[pl.ds(row0, W)], b_s.at[2], b_r.at[2], 1)
    b_own.start()
    b_copies.append(b_own)

    for wdst, wsrc in ((wtsb, w_tsb), (wteb, w_teb)):
        wdst[0:4] = wsrc[...].astype(F32)
        wdst[4:8] = jnp.zeros((4, N), F32)
    mk = mask_ref[x].astype(F32)
    mkb = mk.astype(BF16)
    ninv[...] = 1.0 / (mm(mkb, mkb, TN) + OPM_EPS)
    mtr[...] = jnp.transpose(mk)
    mcb[...] = (mk - 1.0) * (MASK_SCALE * LOG2E)
    mrb[...] = jnp.transpose(mcb[...])
    res_bias = (res_ref[pl.ds(x, 1), :].astype(F32) - 1.0) * (MASK_SCALE * LOG2E)
    mrs[...] = jnp.transpose(jnp.broadcast_to(res_bias, (N, N)))
    def mask_tables(p, carry):
        slot = jnp.where(p < 16, x, ox)
        mrow[p] = pltpu.roll(mrb[...], (N - (2 * slot + c) * B - 2 * (p % 16)) % N, 1)
        mcol[p] = pltpu.roll(mcb[...], (N - (2 * (p // 16) + c) * B - 2 * (p % 16)) % N, 1)
        return carry
    lax.fori_loop(0, B, mask_tables, 0)
    for e in range(B):
        ctf[pl.ds(e * COL_PITCH, B)] = w_oo[B * e:B * e + B].astype(F32)
    def perm_oo(f, carry):
        xf0[rows_at(B * f, B)] = ctf[pl.ds(f, B, stride=COL_PITCH), :]
        return carry
    lax.fori_loop(0, B, perm_oo, 0)
    for t in range(8):
        woot[:, N * t:N * t + N] = jnp.transpose(xf0[N * t:N * t + N, :]).astype(BF16)

    for cpy in b_copies:
        cpy.wait_recv()
    bbf[...] = bb[0:K1].astype(F32) * LOG2E
    for h in range(8):
        bt[h] = jnp.transpose(bbf[pl.ds(h, N, stride=8), :])

    cp_m.wait()

    def x_chunk(ch):
        k = jnp.where(ch < 4, x, ox)
        rows = rows_at(k * B + (ch % 4) * 8, 8)
        return remote(rs.at[rows], xx.at[c, rows], x_s.at[ch], x_r.at[ch], 1)

    def row_seq(p):
        return jnp.where(p < 16, x, ox) * B + 2 * (p % 16)

    def row_x(p):
        s = row_seq(p)
        return ms[s // B, pl.ds(s % B, 2)].reshape(W, W).astype(F32)

    def lane_mask(ref, p, u):
        return jnp.broadcast_to(ref[p][:, u:u + 1], (N, N))

    def row_emit(p, slot, new):
        s = row_seq(p)
        new = new.reshape(2, 2, 2, B, W)
        even, odd = new[:, :, 0], new[:, :, 1]
        xx[c, pl.ds(s, 2)] = jnp.where(c == 0, even, odd).astype(BF16)
        rs[pl.ds(s, 2)] = jnp.where(c == 0, odd, even).astype(BF16)

    row = Attention(st, w_row, w_row_o, 8, row_x, lambda h: bt[h],
                    lambda p, u: lane_mask(mrow, p, u), row_emit)

    def row_four(t, carry):
        @pl.when(jnp.logical_and(t >= 3, t < 7))
        def _():
            m_chunk(2 * t - 6).wait_recv()
            m_chunk(2 * t - 5).wait_recv()

        for e in range(4):
            row.step(4 * t + e, e, 31)

        @pl.when(t > 0)
        def _():
            x_chunk(t - 1).start()
        return carry
    row.begin()
    lax.fori_loop(0, 8, row_four, 0)
    row.end(31)
    x_chunk(7).start()

    def x_wait(ch, carry):
        x_chunk(ch).wait_recv()
        return carry
    lax.fori_loop(0, 8, x_wait, 0)

    def mo_copies(q):
        out = []
        res0 = pl.multiple_of((2 * q + c) * B, B)
        for flip in range(4):
            src = mo.at[pl.ds(peer(flip) * B, B), q]
            dst = m_out.at[x, :, pl.ds(res0, B)]
            if flip == 0:
                out.append(pltpu.make_async_copy(src, dst, mo_l.at[q]))
            else:
                out.append(remote(src, dst, mo_s.at[q, flip - 1], mo_r.at[q, flip - 1], flip))
        return out

    def c_copy(q):
        rows = rows_at((2 * q + c) * K1, K1)
        return remote(ctx.at[rows], ctx.at[rows], c_s.at[q], c_r.at[q], 1)

    def col_x(p):
        return jnp.concatenate([
            jnp.concatenate([ref[pl.ds(2 * p + u, N, stride=COL_PITCH), :] for ref in (xf0, xf1)], axis=1)
            for u in range(2)], axis=0)

    def col_chunk(q, carry):
        for c2 in range(2):
            for k in range(2):
                for r in range(B):
                    v = xx[c2, k * B + r, q].astype(F32)
                    rows = pl.ds(((2 * k + c2) * B + r) * COL_PITCH, B)
                    xf0[rows] = v[:, :N]
                    xf1[rows] = v[:, N:]

        def col_post(p, slot):
            ac = mm(w_ac[...], layer_norm(nw[slot].astype(F32)), NT).astype(BF16).astype(F32)
            for u in range(2):
                loc = q * B + 2 * p + u
                nat = (2 * q + c) * B + 2 * p + u
                acm = (ac[:, N * u:N * u + N] * mtr[pl.ds(nat, 1), :]).astype(BF16)
                at[rows_at(loc * B, B)] = acm[0:B]
                ctx[rows_at(nat * B, B)] = acm[B:2 * B]

        def col_emit(p, slot, new):
            nw[slot] = new.astype(BF16)
            for u in range(2):
                of0[pl.ds(2 * p + u, N, stride=COL_PITCH), :] = new[N * u:N * u + N, :N]
                of1[pl.ds(2 * p + u, N, stride=COL_PITCH), :] = new[N * u:N * u + N, N:]

        col = Attention(st, w_col, w_col_o, 8, col_x, lambda h: None,
                        lambda p, u: lane_mask(mcol, q * 16 + p, u), col_emit, col_post)

        def col_four(t, carry2):
            for e in range(4):
                col.step(4 * t + e, e, 15)
            return carry2
        col.begin()
        lax.fori_loop(0, 4, col_four, 0)
        col.end(15)
        for r in range(N):
            rows = pl.ds(r * COL_PITCH, B)
            mo[r, q] = jnp.concatenate([of0[rows, :], of1[rows, :]], axis=1).astype(BF16)
        c_copy(q).start()
        for cpy in mo_copies(q):
            cpy.start()
        return carry
    lax.fori_loop(0, 2, col_chunk, 0)

    for q in range(2):
        c_copy(q).wait_recv()
    for j in range(N):
        ctf[pl.ds(j * COL_PITCH, B)] = ctx[B * j:B * j + B].astype(F32)

    def perm_c(f, carry):
        cp[rows_at(f * N, N)] = ctf[pl.ds(f, N, stride=COL_PITCH), :].astype(BF16)
        return carry
    lax.fori_loop(0, B, perm_c, 0)
    z_copy.wait_recv()

    def opm_place(ib):
        k, r0 = ib // 4, (ib % 4) * 8
        return k, r0, (2 * k + c) * B + r0

    def opm_outer(ib, slot, fp):
        nat0 = opm_place(ib)[2]
        o = mm(at[rows_at(ib * W, W)], cp[fp * W:fp * W + W], NT)
        for i in range(8):
            nrow = ninv[pl.ds(nat0 + i, 1), :]
            for ff in range(2):
                blk = o[B * i:B * i + B, N * ff:N * ff + N] * nrow
                rr[slot, i, fp * 64 + B * ff:fp * 64 + B * ff + B] = blk.astype(BF16)

    def pair_place(p):
        return p // 16, 2 * (p % 16)

    def opm_product(slot, ip, us):
        ut[us] = mm(woot[...], jnp.concatenate([rr[slot, 2 * ip], rr[slot, 2 * ip + 1]], axis=1), NN)

    def opm_update(p, us):
        k, r = pair_place(p)
        upd = jnp.concatenate([jnp.transpose(ut[us, :, :N]), jnp.transpose(ut[us, :, N:])], axis=0)
        zn = (zr[k, pl.ds(r, 2)].reshape(W, N).astype(F32) + upd).astype(BF16)
        nw[us, :, 0:N] = zn
        ms[k, pl.ds(r, 2), :, 0:N] = zn.reshape(2, N, N)

    def opm_bias(p, us):
        k, r = pair_place(p)
        b = mm(wtsb[...].astype(BF16), layer_norm(nw[us, :, 0:N].astype(F32)), NT)
        bs[rows_at(((2 * k + c) * B + r) * 8, 16)] = side_by_side(b).astype(BF16).astype(F32)

    def opm_two(t, carry):
        for e in range(8):
            p = 8 * t + e
            slot = e // 4
            opm_bias(jnp.maximum(p - 2, 0), e % 2)
            opm_update(jnp.maximum(p - 1, 0), 1 - e % 2)
            nxt = jnp.minimum(2 * t + slot + 1, 7)
            for f in range(4):
                opm_outer(nxt, 1 - slot, e % 4 * 4 + f)
            opm_product(slot, e % 4, e % 2)
        return carry
    for fp in range(16):
        opm_outer(0, 0, fp)
    lax.fori_loop(0, 4, opm_two, 0)
    opm_update(31, 1)
    opm_bias(30, 0)
    opm_bias(31, 1)

    def tri_bias_copies(ref, s_sem, r_sem):
        out = []
        for k in range(2):
            rows = rows_at((2 * k + c) * W, W)
            out.append(remote(ref.at[rows], ref.at[rows], s_sem.at[k], r_sem.at[k], 1))
        return out
    bs_copies = tri_bias_copies(bs, bs_s, bs_r)
    for cpy in bs_copies:
        cpy.start()
    for cpy in bs_copies:
        cpy.wait_recv()
    mres = mrs[...]
    for h in range(4):
        bts[h] = jnp.transpose(bs[pl.ds(h, N, stride=8), :]) * LOG2E + mres

    def zx_copy(ob):
        rows = rows_at(ob * 8, 8)
        return remote(zs.at[rows], zx.at[c, rows], zx_s.at[ob], zx_r.at[ob], 1)

    def ts_x(p):
        return ms[p // 16, pl.ds(2 * (p % 16), 2), :, 0:N].reshape(W, N).astype(F32)

    def ts_post(p, slot):
        b = mm(wteb[...].astype(BF16), layer_norm(nw[slot, :, 0:N].astype(F32)), NT)
        nat = (2 * (p // 16) + c) * B + 2 * (p % 16)
        be[rows_at(nat * 8, 16)] = side_by_side(b).astype(BF16).astype(F32)

    def ts_emit(p, slot, new):
        nw[slot, :, 0:N] = new.astype(BF16)
        new = new.reshape(2, 2, 2, B, N)
        even, odd = new[:, :, 0], new[:, :, 1]
        zx[c, pl.ds(2 * p, 2)] = jnp.where(c == 0, even, odd).astype(BF16)
        zs[pl.ds(2 * p, 2)] = jnp.where(c == 0, odd, even).astype(BF16)

    ts = Attention(st, w_ts, w_ts_o, 4, ts_x, lambda h: bts[h], lambda p, u: None, ts_emit, ts_post)

    def ts_four(ob, carry):
        for e in range(4):
            ts.step(4 * ob + e, e, 31)

        @pl.when(ob > 0)
        def _():
            zx_copy(ob - 1).start()
        return carry
    ts.begin()
    lax.fori_loop(0, 8, ts_four, 0)
    ts.end(31)
    zx_copy(7).start()
    be_copies = tri_bias_copies(be, be_s, be_r)
    for cpy in be_copies:
        cpy.start()
    for cpy in be_copies:
        cpy.wait_recv()
    for h in range(4):
        bte[h] = be[pl.ds(h, N, stride=8), :] * LOG2E + mres

    def zx_wait(ob, carry):
        zx_copy(ob).wait_recv()
        return carry
    lax.fori_loop(0, 8, zx_wait, 0)

    def zo_copies(ci, q, hf):
        out = []
        col0 = pl.multiple_of((2 * q + c) * B + hf * 16, 16)
        h16 = pl.multiple_of(hf * 16, 16)
        for flip in range(4):
            home = peer(flip)
            src = zo.at[pl.ds(home * B, B), q, pl.ds(h16, 16)]
            dst = z_out.at[x, :, pl.ds(col0, 16)]
            if flip == 0:
                out.append(pltpu.make_async_copy(src, dst, zo_l.at[ci]))
            else:
                out.append(remote(src, dst, zo_s.at[ci, flip - 1], zo_r.at[ci, flip - 1], flip))
        return out

    def te_chunk(ci, carry):
        q = ci // 2
        hf = ci % 2
        h16 = pl.multiple_of(hf * 16, 16)
        for c2 in range(2):
            for k in range(2):
                for r in range(B):
                    rows = pl.ds(((2 * k + c2) * B + r) * TRI_PITCH, 16)
                    zf[rows] = zx[c2, k * B + r, q, pl.ds(h16, 16), :].astype(F32)

        def te_x(p):
            return jnp.concatenate([zf[pl.ds(2 * p + u, N, stride=TRI_PITCH), :] for u in range(2)], axis=0)

        def te_emit(p, slot, new):
            for u in range(2):
                zof[pl.ds(2 * p + u, N, stride=TRI_PITCH), :] = new[N * u:N * u + N]

        te = Attention(st, w_te, w_te_o, 4, te_x, lambda h: bte[h], lambda p, u: None, te_emit)

        def te_four(t, carry2):
            for e in range(4):
                te.step(4 * t + e, e, 7)
            return carry2
        te.begin()
        lax.fori_loop(0, 2, te_four, 0)
        te.end(7)
        for r in range(N):
            zo[r, q, pl.ds(h16, 16), :] = zof[pl.ds(r * TRI_PITCH, 16), :].astype(BF16)
        for cpy in zo_copies(ci, q, hf):
            cpy.start()
        return carry
    lax.fori_loop(0, 4, te_chunk, 0)

    for cpy in b_copies + bs_copies + be_copies + [z_copy]:
        cpy.wait_send()
    def drain8(j, carry):
        m_chunk(j).wait_send()
        zx_copy(j).wait_send()
        x_chunk(j).wait_send()
        return carry
    lax.fori_loop(0, 8, drain8, 0)
    for q in range(2):
        c_copy(q).wait_send()
        for cpy in mo_copies(q):
            cpy.wait()
    def drain4(ci, carry):
        for cpy in zo_copies(ci, ci // 2, ci % 2):
            cpy.wait()
        return carry
    lax.fori_loop(0, 4, drain4, 0)


def weight_t(w):
    return w.reshape(w.shape[0], -1).T


def solution(mesh):
    rows_spec = P(PART_AXIS, GROUP_AXIS, None, None)
    in_specs = (rows_spec, rows_spec, P(PART_AXIS, None, None), P(PART_AXIS, None)) + (P(),) * 13

    def block(m, z, mask, res_mask, *weights):
        (w_row_bias, w_row_qkvg, w_row_out, w_col_qkvg, w_col_out, w_opm_ac, w_opm_out,
         w_ts_bias, w_ts_qkvg, w_ts_out, w_te_bias, w_te_qkvg, w_te_out) = weights
        args = (m, z, mask, res_mask, w_row_bias.T, w_ts_bias.T, w_te_bias.T,
                weight_t(w_row_qkvg), w_row_out.reshape(W, W), weight_t(w_col_qkvg), w_col_out.reshape(W, W),
                weight_t(w_opm_ac), w_opm_out.reshape(K1, N),
                weight_t(w_ts_qkvg), w_ts_out.reshape(N, N), weight_t(w_te_qkvg), w_te_out.reshape(N, N))
        vm = pl.BlockSpec(memory_space=pltpu.VMEM)
        hbm = pl.BlockSpec(memory_space=pl.ANY)
        V = pltpu.VMEM
        row_z, row_m, sq = (B, N, N), (B, N, W), (N, N)
        scratch = [V(shape, BF16) for shape in (
            (2,) + row_z, row_z, (2,) + row_m, (2, 64, 2, B, W), (64, 2, B, W), (1280, N))]
        scratch += [V(shape, F32) for shape in (
            (K1, N), (8,) + sq) + ((N * COL_PITCH, N),) * 4]
        scratch += [V((N, 2, B, W), BF16), V((2048, N), BF16), V((B * N, N), BF16), V((N * COL_PITCH, N), F32),
                    V((B * N, N), BF16), V(sq, F32), V(sq, F32), V((N, K1), BF16), V((2, 8, K1, N), BF16)]
        scratch += [V(shape, F32) for shape in ((K1, N), (4,) + sq, (K1, N), (4,) + sq)]
        scratch += [V((2, 64, 2, B, N), BF16), V((64, 2, B, N), BF16), V((N * TRI_PITCH, N), F32), V((N * TRI_PITCH, N), F32),
                    V((N, 2, B, N), BF16)]
        scratch += [V((2, W, W), BF16)] * 2 + [V((4, W, W), BF16), V((4, W, W), F32), V((2, 16) + sq, F32),
                    V((2, 16, N), F32), V((2, W, W), BF16), V((2, W, W), BF16), V((8, N), F32), V((8, N), F32)]
        scratch += [V(sq, F32)] * 3 + [V((B,) + sq, F32)] * 2 + [V((2, N, W), F32)]
        S = pltpu.SemaphoreType.DMA
        scratch += [S(shape) for shape in (
            (3,), (8,), (8,), (1,), (1,), (3,), (3,), (8,), (8,), (2, 3), (2, 3), (2,), (2,), (2,),
            (2,), (2,), (2,), (2,), (8,), (8,), (4, 3), (4, 3), (4,))]
        return pl.pallas_call(
            mega,
            out_shape=(jax.ShapeDtypeStruct(m.shape, BF16), jax.ShapeDtypeStruct(z.shape, BF16)),
            in_specs=[hbm, hbm] + [vm] * 15,
            out_specs=(hbm, hbm),
            scratch_shapes=scratch,
            compiler_params=pltpu.CompilerParams(collective_id=0, has_side_effects=True,
                                                 vmem_limit_bytes=62 << 20),
            name='evoformer_block',
        )(*args)

    return jax.shard_map(block, mesh=mesh, in_specs=in_specs, out_specs=(rows_spec, rows_spec), check_vma=False)
```

```python
import functools

import jax
import jax.numpy as jnp
from jax import lax
from jax.experimental import pallas as pl
from jax.experimental.pallas import tpu as pltpu
from jax.sharding import PartitionSpec as P

F32 = jnp.float32
BF16 = jnp.bfloat16
MASK_SCALE = 10000.0
LN_EPS = 1e-5
OPM_EPS = 1e-3
LOG2E = 1.4426950408889634
HEAD_DIM = 32
N = 128
B = 32
W = 256
K1 = 1024
T16 = 16
COL_PITCH = 40
TRI_PITCH = 24
SCALE2 = (HEAD_DIM ** -0.5) * LOG2E
PART_AXIS = 'data'
GROUP_AXIS = 'dap'
MESH_ID = pl.DeviceIdType.MESH
NT = (((1,), (1,)), ((), ()))
NN = (((1,), (0,)), ((), ()))
TN = (((0,), (0,)), ((), ()))


def mm(lhs, rhs, dims):
    return lax.dot_general(lhs, rhs, dims, preferred_element_type=F32)


def layer_norm(xf):
    mean = jnp.mean(xf, axis=-1, keepdims=True)
    cen = xf - mean
    var = jnp.mean(cen * cen, axis=-1, keepdims=True)
    return (cen * lax.rsqrt(var + LN_EPS)).astype(BF16)


class Attention:
    def __init__(self, st, wt_ref, wo_ref, n_heads, load_x, bias_of, mask_of, emit, post=None):
        self.qs, self.ks, self.vs, self.gs, self.lg, self.mx, self.os = st
        self.wt, self.wo, self.n_heads, self.hd = wt_ref, wo_ref, n_heads, n_heads * HEAD_DIM
        self.load_x, self.bias_of, self.mask_of, self.emit, self.post = load_x, bias_of, mask_of, emit, post
        self.items = [(u, h) for u in range(2) for h in range(0, n_heads, 2)]

    def p_part(self, y, i, part):
        hd = self.hd
        w = self.wt[part * hd:(part + 1) * hd]
        if part == 0:
            self.qs[i % 2, 0:hd] = mm(w, y, NT).astype(BF16)
        elif part == 1:
            self.ks[i % 2, :, 0:hd] = mm(y, w, NT).astype(BF16)
        elif part == 2:
            self.vs[i % 4, 0:hd] = mm(w, y, NT).astype(BF16)
        else:
            self.gs[i % 4, 0:hd] = jax.nn.sigmoid(mm(w, y, NT))

    def l_part(self, p, i, item):
        u, h = item
        tok = slice(N * u, N * u + N)
        blocks = []
        for hh in (h, h + 1):
            h4 = hh % 4
            rows = [self.qs[i % 2, B * hh:B * hh + B, tok]]
            if h4 > 0:
                rows.insert(0, jnp.zeros((B * h4, N), BF16))
            if h4 < 3:
                rows.append(jnp.zeros((N - B - B * h4, N), BF16))
            blocks.append(jnp.concatenate(rows, axis=0))
        g0 = h // 4 * N
        logits = mm(self.ks[i % 2, tok, g0:g0 + N], jnp.concatenate(blocks, axis=1), NN)
        mask_col = self.mask_of(p, u)
        for n, hh in enumerate((h, h + 1)):
            lg = logits[:, N * n:N * n + N] * SCALE2
            bias = self.bias_of(hh)
            if bias is not None:
                lg = lg + bias
            if mask_col is not None:
                lg = lg + mask_col
            row = u * self.n_heads + hh
            self.lg[i % 2, row] = lg
            self.mx[i % 2, row:row + 1] = jnp.max(lg, axis=0, keepdims=True)

    def s_part(self, i, item):
        u, h = item
        tok = slice(N * u, N * u + N)
        ps, inv = [], []
        for hh in (h, h + 1):
            row = u * self.n_heads + hh
            ex = jnp.exp2(self.lg[i % 2, row] - self.mx[i % 2, row:row + 1])
            inv.append(1.0 / jnp.sum(ex, axis=0, keepdims=True))
            ps.append(ex.astype(BF16))
        h0 = h * B
        ov = mm(self.vs[i % 4, h0:h0 + 2 * B, tok], jnp.concatenate(ps, axis=1), NN)
        o = jnp.concatenate([ov[0:B, 0:N] * inv[0], ov[B:2 * B, N:W] * inv[1]], axis=0)
        self.os[i % 2, h0:h0 + 2 * B, tok] = (o * self.gs[i % 4, h0:h0 + 2 * B, tok]).astype(BF16)

    def o_part(self, p, i):
        self.emit(p, i % 2, self.load_x(p) + mm(self.os[i % 2, 0:self.hd], self.wo[...], TN))

    def step(self, p, i, last):
        if self.post is not None:
            self.post(jnp.maximum(p - 2, 0), i % 2)
        self.o_part(jnp.maximum(p - 1, 0), i - 1)
        y = layer_norm(self.load_x(jnp.minimum(p + 2, last)))
        nxt = jnp.minimum(p + 1, last)
        for n, item in enumerate(self.items):
            self.l_part(nxt, i + 1, item)
            self.s_part(i, item)
            for part in range(4):
                if part * len(self.items) // 4 == n:
                    self.p_part(y, i + 2, part)

    def begin(self):
        for i in range(2):
            y = layer_norm(self.load_x(i))
            for part in range(4):
                self.p_part(y, i, part)
        for item in self.items:
            self.l_part(0, 0, item)

    def end(self, last):
        self.o_part(last, 3)
        if self.post is not None:
            self.post(last - 1, 0)
            self.post(last, 1)


def rows_at(start, size):
    return pl.ds(pl.multiple_of(start, size), size)


def side_by_side(b):
    return jnp.concatenate([b[:, :N], b[:, N:]], axis=0)


def mega(m_in, z_in, mask_ref, res_ref, w_rb, w_tsb, w_teb, w_row, w_row_o, w_col, w_col_o, w_ac, w_oo,
         w_ts, w_ts_o, w_te, w_te_o, m_out, z_out,
         zr, zot, ms, xx, rst, bbx, bbo, bbf, bt, xf0, xf1, of0, of1, mo, at, ctx, ctf, cp, ninv, mtr, woot, rr,
         bs, bts, be, bte, zx, zs, zf, zof, zo, qs, ks, vs, gs, lgs, mxs, ots, nw, wtsb, wteb, mcb, mrb, mrs, mrow, mcol, ut,
         l_sem, zi_s, zi_r, b_s, b_r, xa_s, xa_r, xb_s, xb_r, mo_s, mo_r, mo_l, c_s, c_r, bs_s, bs_r, be_s, be_r,
         zx_s, zx_r, zo_s, zo_r, zo_l):
    st = (qs, ks, vs, gs, lgs, mxs, ots)
    dat = lax.axis_index(PART_AXIS)
    dev = lax.axis_index(GROUP_AXIS)
    x = dev // 2
    c = dev % 2
    ox = 1 - x

    def peer(flip):
        px = ox if flip >= 2 else x
        pc = (1 - c) if flip % 2 else c
        return px * 2 + pc

    def remote(src, dst, s_sem, r_sem, flip):
        return pltpu.make_async_remote_copy(src, dst, s_sem, r_sem, device_id=(dat, peer(flip)),
                                            device_id_type=MESH_ID)

    barrier = pltpu.get_barrier_semaphore()
    for flip in (1, 2, 3):
        pl.semaphore_signal(barrier, inc=1, device_id=(dat, peer(flip)), device_id_type=MESH_ID)
    cp_zo = pltpu.make_async_copy(z_in.at[ox], zot, l_sem.at[0])
    cp_zr = pltpu.make_async_copy(z_in.at[x], zr.at[x], l_sem.at[1])
    cp_mo = pltpu.make_async_copy(m_in.at[ox], ms.at[ox], l_sem.at[2])
    cp_mx = pltpu.make_async_copy(m_in.at[x], ms.at[x], l_sem.at[3])
    for cpy in (cp_zr, cp_zo, cp_mo, cp_mx):
        cpy.start()
    pl.semaphore_wait(barrier, 3)

    z_copies = []
    for n, (first, size) in enumerate(((0, 4), (4, 8), (12, 20))):
        rows = pl.ds(first, size)
        z_copies.append(remote(z_in.at[ox, rows], zr.at[x, rows], zi_s.at[n], zi_r.at[n], 2))
    z_copies[0].start()

    row0 = pl.multiple_of(dev * W, W)
    own = pl.ds(row0, W)

    def bias_rows(load, dst):
        def body(g, carry):
            for p in range(4):
                y = layer_norm(load(8 * g + 2 * p).reshape(W, N).astype(F32))
                dst[rows_at(row0 + 64 * g + T16 * p, T16)] = side_by_side(mm(w_rb[...], y, NT)).astype(BF16)
            return carry
        lax.fori_loop(0, 4, body, 0)

    b_copies = [remote(src.at[own], dst.at[own], b_s.at[n], b_r.at[n], flip) for n, (src, dst, flip) in enumerate((
        (bbx, bbo, 2), (bbx, bbo, 3), (bbo, bbo, 1), (bbo, bbx, 2), (bbo, bbx, 3), (bbx, bbx, 1)))]
    cp_zr.wait()
    bias_rows(lambda r: zr[x, pl.ds(r, 2)], bbx)
    for cpy in b_copies[:2]:
        cpy.start()
    cp_zo.wait()
    bias_rows(lambda r: zot[pl.ds(r, 2)], bbo)
    for cpy in b_copies[2:]:
        cpy.start()
    z_copies[1].start()

    for wdst, wsrc in ((wtsb, w_tsb), (wteb, w_teb)):
        wdst[0:4] = wsrc[...].astype(F32)
        wdst[4:8] = jnp.zeros((4, N), F32)
    mk = mask_ref[x].astype(F32)
    mkb = mk.astype(BF16)
    ninv[...] = 1.0 / (mm(mkb, mkb, TN) + OPM_EPS)
    mtr[...] = jnp.transpose(mk)
    mcb[...] = (mk - 1.0) * (MASK_SCALE * LOG2E)
    mrb[1] = jnp.transpose(mcb[...])
    mrb[0] = jnp.transpose((mask_ref[ox].astype(F32) - 1.0) * (MASK_SCALE * LOG2E))
    res_bias = (res_ref[pl.ds(x, 1), :].astype(F32) - 1.0) * (MASK_SCALE * LOG2E)
    mrs[...] = jnp.transpose(jnp.broadcast_to(res_bias, (N, N)))
    def mask_tables(p, carry):
        mrow[p] = pltpu.roll(mrb[p // T16], (N - dev * B - 2 * (p % T16)) % N, 1)
        mcol[p] = pltpu.roll(mcb[...], (N - (2 * (p // T16) + c) * B - 2 * (p % T16)) % N, 1)
        return carry
    lax.fori_loop(0, B, mask_tables, 0)
    for e in range(B):
        ctf[pl.ds(e * COL_PITCH, B)] = w_oo[B * e:B * e + B].astype(F32)
    def perm_oo(f, carry):
        xf0[rows_at(B * f, B)] = ctf[pl.ds(f, B, stride=COL_PITCH), :]
        return carry
    lax.fori_loop(0, B, perm_oo, 0)
    for t in range(8):
        woot[:, N * t:N * t + N] = jnp.transpose(xf0[N * t:N * t + N, :]).astype(BF16)

    def bias_table(n, src):
        for cpy in b_copies[3 * n:3 * n + 3]:
            cpy.wait_recv()
        bbf[...] = src[...].astype(F32) * LOG2E
        for h in range(8):
            bt[n, h] = jnp.transpose(bbf[pl.ds(h, N, stride=8), :])
    bias_table(0, bbo)

    cp_mo.wait()
    cp_mx.wait()

    def xa_copy(q, t, rel):
        rows = rows_at(t * 8, 8)
        return remote(rst.at[rel, rows, q], xx.at[1 + rel, rows, q], xa_s.at[q, t, rel], xa_r.at[q, t, rel], 2 + rel)

    def xb_copy(t):
        return remote(rst.at[1, rows_at(B + t * 8, 8)], xx.at[0, rows_at(t * 8, 8)], xb_s.at[t], xb_r.at[t], 1)

    def row_x(p):
        return ms[jnp.where(p < T16, ox, x), pl.ds(2 * (p % T16), 2)].reshape(W, W).astype(F32)

    def lane_mask(ref, p, u):
        return jnp.broadcast_to(ref[p][:, u:u + 1], (N, N))

    def row_emit(p, slot, new):
        new = new.reshape(2, 2, 2, B, W)
        even, odd = new[:, :, 0], new[:, :, 1]
        rst[0, pl.ds(2 * p, 2)] = jnp.where(c == 0, even, odd).astype(BF16)
        rst[1, pl.ds(2 * p, 2)] = jnp.where(c == 0, odd, even).astype(BF16)

    def row_four(t, carry):
        @pl.when(t == 3)
        def _():
            bias_table(1, bbx)

        def bias_at(p):
            return lambda h: bt[jnp.minimum(p + 1, 31) // T16, h]

        for e in range(4):
            row = Attention(st, w_row, w_row_o, 8, row_x, bias_at(4 * t + e),
                            lambda p, u: lane_mask(mrow, p, u), row_emit)
            row.step(4 * t + e, e, 31)

        @pl.when(jnp.logical_and(t > 0, t < 5))
        def _():
            for rel in range(2):
                xa_copy(0, t - 1, rel).start()

        @pl.when(t == 4)
        def _():
            for tt in range(4):
                for rel in range(2):
                    xa_copy(1, tt, rel).start()
            z_copies[2].start()

        @pl.when(t > 4)
        def _():
            xb_copy(t - 5).start()
        return carry
    row = Attention(st, w_row, w_row_o, 8, row_x, lambda h: bt[0, h], lambda p, u: lane_mask(mrow, p, u), row_emit)
    row.begin()
    lax.fori_loop(0, 8, row_four, 0)
    row.end(31)
    xb_copy(3).start()
    for t in range(4):
        xb_copy(t).wait_recv()

    def mo_copies(q):
        out = []
        res0 = pl.multiple_of((2 * q + c) * B, B)
        for flip in range(4):
            src = mo.at[pl.ds(peer(flip) * B, B), q]
            dst = m_out.at[x, :, pl.ds(res0, B)]
            if flip == 0:
                out.append(pltpu.make_async_copy(src, dst, mo_l.at[q]))
            else:
                out.append(remote(src, dst, mo_s.at[q, flip - 1], mo_r.at[q, flip - 1], flip))
        return out

    def c_copy(q):
        rows = rows_at((2 * q + c) * K1, K1)
        return remote(ctx.at[rows], ctx.at[rows], c_s.at[q], c_r.at[q], 1)

    def col_x(p):
        return jnp.concatenate([
            jnp.concatenate([ref[pl.ds(2 * p + u, N, stride=COL_PITCH), :] for ref in (xf0, xf1)], axis=1)
            for u in range(2)], axis=0)

    def col_chunk(q, carry):
        for t in range(4):
            for rel in range(2):
                xa_copy(q, t, rel).wait_recv()
        for flip in range(4):
            base = peer(flip) * (B * COL_PITCH)
            for r in range(B):
                v = (xx[flip - 1, r, q] if flip else rst[0, B + r, q]).astype(F32)
                rows = pl.ds(pl.multiple_of(base + r * COL_PITCH, 8), B)
                xf0[rows] = v[:, :N]
                xf1[rows] = v[:, N:]

        def col_post(p, slot):
            ac = mm(w_ac[...], layer_norm(nw[slot].astype(F32)), NT).astype(BF16).astype(F32)
            for u in range(2):
                loc = q * B + 2 * p + u
                nat = (2 * q + c) * B + 2 * p + u
                acm = (ac[:, N * u:N * u + N] * mtr[pl.ds(nat, 1), :]).astype(BF16)
                at[rows_at(loc * B, B)] = acm[0:B]
                ctx[rows_at(nat * B, B)] = acm[B:2 * B]

        def col_emit(p, slot, new):
            nw[slot] = new.astype(BF16)
            for u in range(2):
                of0[pl.ds(2 * p + u, N, stride=COL_PITCH), :] = new[N * u:N * u + N, :N]
                of1[pl.ds(2 * p + u, N, stride=COL_PITCH), :] = new[N * u:N * u + N, N:]

        col = Attention(st, w_col, w_col_o, 8, col_x, lambda h: None,
                        lambda p, u: lane_mask(mcol, q * T16 + p, u), col_emit, col_post)

        def col_four(t, carry2):
            for e in range(4):
                col.step(4 * t + e, e, 15)
            return carry2
        col.begin()
        lax.fori_loop(0, 4, col_four, 0)
        col.end(15)
        for r in range(N):
            rows = pl.ds(r * COL_PITCH, B)
            mo[r, q] = jnp.concatenate([of0[rows, :], of1[rows, :]], axis=1).astype(BF16)
        c_copy(q).start()
        for cpy in mo_copies(q):
            cpy.start()
        return carry
    lax.fori_loop(0, 2, col_chunk, 0)

    for q in range(2):
        c_copy(q).wait_recv()
    for j in range(N):
        ctf[pl.ds(j * COL_PITCH, B)] = ctx[B * j:B * j + B].astype(F32)

    def perm_c(f, carry):
        cp[rows_at(f * N, N)] = ctf[pl.ds(f, N, stride=COL_PITCH), :].astype(BF16)
        return carry
    lax.fori_loop(0, B, perm_c, 0)
    for cpy in z_copies:
        cpy.wait_recv()

    def opm_place(ib):
        k, r0 = ib // 4, (ib % 4) * 8
        return k, r0, (2 * k + c) * B + r0

    def opm_outer(ib, slot, fp):
        nat0 = opm_place(ib)[2]
        o = mm(at[rows_at(ib * W, W)], cp[fp * W:fp * W + W], NT)
        for i in range(8):
            nrow = ninv[pl.ds(nat0 + i, 1), :]
            for ff in range(2):
                blk = o[B * i:B * i + B, N * ff:N * ff + N] * nrow
                rr[slot, i, fp * 64 + B * ff:fp * 64 + B * ff + B] = blk.astype(BF16)

    def pair_place(p):
        return p // T16, 2 * (p % T16)

    def opm_product(slot, ip, us):
        ut[us] = mm(woot[...], jnp.concatenate([rr[slot, 2 * ip], rr[slot, 2 * ip + 1]], axis=1), NN)

    def opm_update(p, us):
        k, r = pair_place(p)
        upd = jnp.concatenate([jnp.transpose(ut[us, :, :N]), jnp.transpose(ut[us, :, N:])], axis=0)
        zn = (zr[k, pl.ds(r, 2)].reshape(W, N).astype(F32) + upd).astype(BF16)
        nw[us, :, 0:N] = zn
        ms[k, pl.ds(r, 2), :, 0:N] = zn.reshape(2, N, N)

    def opm_bias(p, us):
        k, r = pair_place(p)
        b = mm(wtsb[...].astype(BF16), layer_norm(nw[us, :, 0:N].astype(F32)), NT)
        bs[rows_at(((2 * k + c) * B + r) * 8, T16)] = side_by_side(b).astype(BF16).astype(F32)

    def opm_two(t, carry):
        for e in range(8):
            p = 8 * t + e
            slot = e // 4
            opm_bias(jnp.maximum(p - 2, 0), e % 2)
            opm_update(jnp.maximum(p - 1, 0), 1 - e % 2)
            nxt = jnp.minimum(2 * t + slot + 1, 7)
            for f in range(4):
                opm_outer(nxt, 1 - slot, e % 4 * 4 + f)
            opm_product(slot, e % 4, e % 2)
        return carry
    for fp in range(T16):
        opm_outer(0, 0, fp)
    lax.fori_loop(0, 4, opm_two, 0)
    opm_update(31, 1)
    opm_bias(30, 0)
    opm_bias(31, 1)

    def tri_bias_copies(ref, s_sem, r_sem):
        out = []
        for k in range(2):
            rows = rows_at((2 * k + c) * W, W)
            out.append(remote(ref.at[rows], ref.at[rows], s_sem.at[k], r_sem.at[k], 1))
        return out
    bs_copies = tri_bias_copies(bs, bs_s, bs_r)
    for cpy in bs_copies:
        cpy.start()
    for cpy in bs_copies:
        cpy.wait_recv()
    mres = mrs[...]
    for h in range(4):
        bts[h] = jnp.transpose(bs[pl.ds(h, N, stride=8), :]) * LOG2E + mres

    def zx_copy(ob):
        rows = rows_at(ob * 8, 8)
        return remote(zs.at[rows], zx.at[c, rows], zx_s.at[ob], zx_r.at[ob], 1)

    def ts_x(p):
        return ms[p // T16, pl.ds(2 * (p % T16), 2), :, 0:N].reshape(W, N).astype(F32)

    def ts_post(p, slot):
        b = mm(wteb[...].astype(BF16), layer_norm(nw[slot, :, 0:N].astype(F32)), NT)
        nat = (2 * (p // T16) + c) * B + 2 * (p % T16)
        be[rows_at(nat * 8, T16)] = side_by_side(b).astype(BF16).astype(F32)

    def ts_emit(p, slot, new):
        nw[slot, :, 0:N] = new.astype(BF16)
        new = new.reshape(2, 2, 2, B, N)
        even, odd = new[:, :, 0], new[:, :, 1]
        zx[c, pl.ds(2 * p, 2)] = jnp.where(c == 0, even, odd).astype(BF16)
        zs[pl.ds(2 * p, 2)] = jnp.where(c == 0, odd, even).astype(BF16)

    ts = Attention(st, w_ts, w_ts_o, 4, ts_x, lambda h: bts[h], lambda p, u: None, ts_emit, ts_post)

    def ts_four(ob, carry):
        for e in range(4):
            ts.step(4 * ob + e, e, 31)

        @pl.when(ob > 0)
        def _():
            zx_copy(ob - 1).start()
        return carry
    ts.begin()
    lax.fori_loop(0, 8, ts_four, 0)
    ts.end(31)
    zx_copy(7).start()
    be_copies = tri_bias_copies(be, be_s, be_r)
    for cpy in be_copies:
        cpy.start()
    for cpy in be_copies:
        cpy.wait_recv()
    for h in range(4):
        bte[h] = be[pl.ds(h, N, stride=8), :] * LOG2E + mres

    def zx_wait(ob, carry):
        zx_copy(ob).wait_recv()
        return carry
    lax.fori_loop(0, 8, zx_wait, 0)

    def zo_copies(ci, q, hf):
        out = []
        col0 = pl.multiple_of((2 * q + c) * B + hf * T16, T16)
        h16 = pl.multiple_of(hf * T16, T16)
        for flip in range(4):
            home = peer(flip)
            src = zo.at[pl.ds(home * B, B), q, pl.ds(h16, T16)]
            dst = z_out.at[x, :, pl.ds(col0, T16)]
            if flip == 0:
                out.append(pltpu.make_async_copy(src, dst, zo_l.at[ci]))
            else:
                out.append(remote(src, dst, zo_s.at[ci, flip - 1], zo_r.at[ci, flip - 1], flip))
        return out

    def te_chunk(ci, carry):
        q = ci // 2
        hf = ci % 2
        h16 = pl.multiple_of(hf * T16, T16)
        for c2 in range(2):
            for k in range(2):
                for r in range(B):
                    rows = pl.ds(((2 * k + c2) * B + r) * TRI_PITCH, T16)
                    zf[rows] = zx[c2, k * B + r, q, pl.ds(h16, T16), :].astype(F32)

        def te_x(p):
            return jnp.concatenate([zf[pl.ds(2 * p + u, N, stride=TRI_PITCH), :] for u in range(2)], axis=0)

        def te_emit(p, slot, new):
            for u in range(2):
                zof[pl.ds(2 * p + u, N, stride=TRI_PITCH), :] = new[N * u:N * u + N]

        te = Attention(st, w_te, w_te_o, 4, te_x, lambda h: bte[h], lambda p, u: None, te_emit)

        def te_four(t, carry2):
            for e in range(4):
                te.step(4 * t + e, e, 7)
            return carry2
        te.begin()
        lax.fori_loop(0, 2, te_four, 0)
        te.end(7)
        for r in range(N):
            zo[r, q, pl.ds(h16, T16), :] = zof[pl.ds(r * TRI_PITCH, T16), :].astype(BF16)
        for cpy in zo_copies(ci, q, hf):
            cpy.start()
        return carry
    lax.fori_loop(0, 4, te_chunk, 0)

    for cpy in b_copies + bs_copies + be_copies + z_copies:
        cpy.wait_send()
    def drain8(j, carry):
        zx_copy(j).wait_send()
        return carry
    lax.fori_loop(0, 8, drain8, 0)
    for t in range(4):
        xb_copy(t).wait_send()
        for rel in range(2):
            xa_copy(0, t, rel).wait_send()
            xa_copy(1, t, rel).wait_send()
    for q in range(2):
        c_copy(q).wait_send()
        for cpy in mo_copies(q):
            cpy.wait()
    def drain4(ci, carry):
        for cpy in zo_copies(ci, ci // 2, ci % 2):
            cpy.wait()
        return carry
    lax.fori_loop(0, 4, drain4, 0)


def weight_t(w):
    return w.reshape(w.shape[0], -1).T


def solution(mesh):
    rows_spec = P(PART_AXIS, GROUP_AXIS, None, None)
    in_specs = (rows_spec, rows_spec, P(PART_AXIS, None, None), P(PART_AXIS, None)) + (P(),) * 13

    def block(m, z, mask, res_mask, *weights):
        (w_row_bias, w_row_qkvg, w_row_out, w_col_qkvg, w_col_out, w_opm_ac, w_opm_out,
         w_ts_bias, w_ts_qkvg, w_ts_out, w_te_bias, w_te_qkvg, w_te_out) = weights
        args = (m, z, mask, res_mask, w_row_bias.T, w_ts_bias.T, w_te_bias.T,
                weight_t(w_row_qkvg), w_row_out.reshape(W, W), weight_t(w_col_qkvg), w_col_out.reshape(W, W),
                weight_t(w_opm_ac), w_opm_out.reshape(K1, N),
                weight_t(w_ts_qkvg), w_ts_out.reshape(N, N), weight_t(w_te_qkvg), w_te_out.reshape(N, N))
        vm = pl.BlockSpec(memory_space=pltpu.VMEM)
        hbm = pl.BlockSpec(memory_space=pl.ANY)
        V = pltpu.VMEM
        row_z, row_m, sq = (B, N, N), (B, N, W), (N, N)
        scratch = [V(shape, BF16) for shape in (
            (2,) + row_z, row_z, (2,) + row_m, (3, B, 2, B, W), (2, 64, 2, B, W), (K1, N), (K1, N))]
        scratch += [V(shape, F32) for shape in (
            (K1, N), (2, 8) + sq) + ((N * COL_PITCH, N),) * 4]
        scratch += [V((N, 2, B, W), BF16), V((2048, N), BF16), V((B * N, N), BF16), V((N * COL_PITCH, N), F32),
                    V((B * N, N), BF16), V(sq, F32), V(sq, F32), V((N, K1), BF16), V((2, 8, K1, N), BF16)]
        scratch += [V(shape, F32) for shape in ((K1, N), (4,) + sq, (K1, N), (4,) + sq)]
        scratch += [V((2, 64, 2, B, N), BF16), V((64, 2, B, N), BF16), V((N * TRI_PITCH, N), F32), V((N * TRI_PITCH, N), F32),
                    V((N, 2, B, N), BF16)]
        scratch += [V((2, W, W), BF16)] * 2 + [V((4, W, W), BF16), V((4, W, W), F32), V((2, T16) + sq, F32),
                    V((2, T16, N), F32), V((2, W, W), BF16), V((2, W, W), BF16), V((8, N), F32), V((8, N), F32)]
        scratch += [V(sq, F32), V((2,) + sq, F32), V(sq, F32)] + [V((B,) + sq, F32)] * 2 + [V((2, N, W), F32)]
        S = pltpu.SemaphoreType.DMA
        scratch += [S(shape) for shape in (
            (4,), (3,), (3,), (6,), (6,), (2, 4, 2), (2, 4, 2), (4,), (4,), (2, 3), (2, 3), (2,), (2,), (2,),
            (2,), (2,), (2,), (2,), (8,), (8,), (4, 3), (4, 3), (4,))]
        return pl.pallas_call(
            mega,
            out_shape=(jax.ShapeDtypeStruct(m.shape, BF16), jax.ShapeDtypeStruct(z.shape, BF16)),
            in_specs=[hbm, hbm] + [vm] * 15,
            out_specs=(hbm, hbm),
            scratch_shapes=scratch,
            compiler_params=pltpu.CompilerParams(collective_id=0, has_side_effects=True,
                                                 vmem_limit_bytes=62 << 20),
            name='evoformer_block',
        )(*args)

    return jax.shard_map(block, mesh=mesh, in_specs=in_specs, out_specs=(rows_spec, rows_spec), check_vma=False)
```

```python
import functools

import jax
import jax.numpy as jnp
from jax import lax
from jax.experimental import pallas as pl
from jax.experimental.pallas import tpu as pltpu
from jax.sharding import PartitionSpec as P

F32 = jnp.float32
BF16 = jnp.bfloat16
MASK_SCALE = 10000.0
LN_EPS = 1e-5
OPM_EPS = 1e-3
LOG2E = 1.4426950408889634
HEAD_DIM = 32
N = 128
B = 32
W = 256
K1 = 1024
T16 = 16
E8 = 8
COL_PITCH = 40
TRI_PITCH = 24
SCALE2 = (HEAD_DIM ** -0.5) * LOG2E
PART_AXIS = 'data'
GROUP_AXIS = 'dap'
MESH_ID = pl.DeviceIdType.MESH
NT = (((1,), (1,)), ((), ()))
NN = (((1,), (0,)), ((), ()))
TN = (((0,), (0,)), ((), ()))


def mm(lhs, rhs, dims):
    return lax.dot_general(lhs, rhs, dims, preferred_element_type=F32)


def layer_norm(xf):
    mean = jnp.mean(xf, axis=-1, keepdims=True)
    cen = xf - mean
    var = jnp.mean(cen * cen, axis=-1, keepdims=True)
    return (cen * lax.rsqrt(var + LN_EPS)).astype(BF16)


class Attention:
    def __init__(self, st, wt_ref, wo_ref, n_heads, load_x, bias_of, mask_of, emit, post=None):
        self.qs, self.ks, self.vs, self.gs, self.lg, self.mx, self.os, self.ys = st
        self.wt, self.wo, self.n_heads, self.hd = wt_ref, wo_ref, n_heads, n_heads * HEAD_DIM
        self.load_x, self.bias_of, self.mask_of, self.emit, self.post = load_x, bias_of, mask_of, emit, post
        self.items = [(u, h) for u in range(2) for h in range(0, n_heads, 2)]

    def n_parts(self, p, i):
        xf = self.load_x(p)
        for b in range(4):
            rows = slice(64 * b, 64 * b + 64)
            self.ys[i % 2, rows, 0:xf.shape[1]] = layer_norm(xf[rows])
            yield

    def p_part(self, i, part):
        hd = self.hd
        y = self.ys[i % 2, :, 0:self.wt.shape[1]]
        w = self.wt[part * hd:(part + 1) * hd]
        if part == 0:
            self.qs[i % 2, 0:hd] = mm(w, y, NT).astype(BF16)
        elif part == 1:
            self.ks[i % 2, :, 0:hd] = mm(y, w, NT).astype(BF16)
        elif part == 2:
            self.vs[i % 4, 0:hd] = mm(w, y, NT).astype(BF16)
        else:
            self.gs[i % 4, 0:hd] = jax.nn.sigmoid(mm(w, y, NT))

    def l_part(self, p, i, item):
        u, h = item
        tok = slice(N * u, N * u + N)
        blocks = []
        for hh in (h, h + 1):
            h4 = hh % 4
            rows = [self.qs[i % 2, B * hh:B * hh + B, tok]]
            if h4 > 0:
                rows.insert(0, jnp.zeros((B * h4, N), BF16))
            if h4 < 3:
                rows.append(jnp.zeros((N - B - B * h4, N), BF16))
            blocks.append(jnp.concatenate(rows, axis=0))
        g0 = h // 4 * N
        logits = mm(self.ks[i % 2, tok, g0:g0 + N], jnp.concatenate(blocks, axis=1), NN)
        mask_col = self.mask_of(p, u)
        for n, hh in enumerate((h, h + 1)):
            lg = logits[:, N * n:N * n + N] * SCALE2
            bias = self.bias_of(hh)
            if bias is not None:
                lg = lg + bias
            if mask_col is not None:
                lg = lg + mask_col
            row = u * self.n_heads + hh
            self.lg[i % 2, row] = lg
            self.mx[i % 2, row:row + 1] = jnp.max(lg, axis=0, keepdims=True)

    def s_part(self, i, item):
        u, h = item
        tok = slice(N * u, N * u + N)
        ps, inv = [], []
        for hh in (h, h + 1):
            row = u * self.n_heads + hh
            ex = jnp.exp2(self.lg[i % 2, row] - self.mx[i % 2, row:row + 1])
            inv.append(1.0 / jnp.sum(ex, axis=0, keepdims=True))
            ps.append(ex.astype(BF16))
        h0 = h * B
        ov = mm(self.vs[i % 4, h0:h0 + 2 * B, tok], jnp.concatenate(ps, axis=1), NN)
        o = jnp.concatenate([ov[0:B, 0:N] * inv[0], ov[B:2 * B, N:W] * inv[1]], axis=0)
        self.os[i % 2, h0:h0 + 2 * B, tok] = (o * self.gs[i % 4, h0:h0 + 2 * B, tok]).astype(BF16)

    def o_part(self, p, i):
        self.emit(p, i % 2, self.load_x(p) + mm(self.os[i % 2, 0:self.hd], self.wo[...], TN))

    def step(self, p, i, last):
        if self.post is not None:
            self.post(jnp.maximum(p - 2, 0), i % 2)
        self.o_part(jnp.maximum(p - 1, 0), i - 1)
        norm = self.n_parts(jnp.minimum(p + 3, last), i + 3)
        nxt = jnp.minimum(p + 1, last)
        for n, item in enumerate(self.items):
            self.l_part(nxt, i + 1, item)
            self.s_part(i, item)
            for part in range(4):
                if part * len(self.items) // 4 == n:
                    next(norm)
                    self.p_part(i + 2, part)

    def begin(self):
        for i in range(3):
            for _ in self.n_parts(i, i):
                pass
            for part in range(4 if i < 2 else 0):
                self.p_part(i, part)
        for item in self.items:
            self.l_part(0, 0, item)

    def end(self, last):
        self.o_part(last, 3)
        if self.post is not None:
            self.post(last - 1, 0)
            self.post(last, 1)


def rows_at(start, size):
    return pl.ds(pl.multiple_of(start, size), size)


def side_by_side(b):
    return jnp.concatenate([b[:, :N], b[:, N:]], axis=0)


def mega(m_in, z_in, mask_ref, res_ref, w_rb, w_tsb, w_teb, w_row, w_row_o, w_col, w_col_o, w_ac, w_oo,
         w_ts, w_ts_o, w_te, w_te_o, m_out, z_out,
         zr, zot, ms, xx, rst, bbx, bbo, bbf, bt, xf0, xf1, of0, of1, mo, at, ctx, ctf, cp, ninv, mtr, woot, rr,
         bs, bts, be, bte, zx, zs, zo, qs, ks, vs, gs, lgs, mxs, ots, ys, nw, wtsb, wteb, mcb, mrb, mrs, mrow, mcol, ut,
         l_sem, zi_s, zi_r, b_s, b_r, xa_s, xa_r, xb_s, xb_r, mo_s, mo_r, mo_l, c_s, c_r, bs_s, bs_r, be_s, be_r,
         zx_s, zx_r, zo_s, zo_r, zo_l):
    st = (qs, ks, vs, gs, lgs, mxs, ots, ys)
    zf, zof = xf1, of1
    dat = lax.axis_index(PART_AXIS)
    dev = lax.axis_index(GROUP_AXIS)
    x = dev // 2
    c = dev % 2
    ox = 1 - x

    def peer(flip):
        px = ox if flip >= 2 else x
        pc = (1 - c) if flip % 2 else c
        return px * 2 + pc

    def remote(src, dst, s_sem, r_sem, flip):
        return pltpu.make_async_remote_copy(src, dst, s_sem, r_sem, device_id=(dat, peer(flip)),
                                            device_id_type=MESH_ID)

    barrier = pltpu.get_barrier_semaphore()
    for flip in (1, 2, 3):
        pl.semaphore_signal(barrier, inc=1, device_id=(dat, peer(flip)), device_id_type=MESH_ID)
    cp_zo = pltpu.make_async_copy(z_in.at[ox], zot, l_sem.at[0])
    cp_zr = pltpu.make_async_copy(z_in.at[x], zr.at[x], l_sem.at[1])
    cp_mo = pltpu.make_async_copy(m_in.at[ox], ms.at[ox], l_sem.at[2])
    cp_mx = pltpu.make_async_copy(m_in.at[x], ms.at[x], l_sem.at[3])
    for cpy in (cp_zr, cp_zo, cp_mo, cp_mx):
        cpy.start()
    pl.semaphore_wait(barrier, 3)

    z_copies = []
    for n, (first, size) in enumerate(((0, E8), (E8, 24))):
        rows = pl.ds(first, size)
        z_copies.append(remote(z_in.at[ox, rows], zr.at[x, rows], zi_s.at[n], zi_r.at[n], 2))

    row0 = pl.multiple_of(dev * W, W)
    own = pl.ds(row0, W)

    def bias_rows(load, dst):
        def body(g, carry):
            for p in range(4):
                y = layer_norm(load(E8 * g + 2 * p).reshape(W, N).astype(F32))
                dst[rows_at(row0 + 64 * g + T16 * p, T16)] = side_by_side(mm(w_rb[...], y, NT)).astype(BF16)
            return carry
        lax.fori_loop(0, 4, body, 0)

    b_copies = [remote(src.at[own], dst.at[own], b_s.at[n], b_r.at[n], flip) for n, (src, dst, flip) in enumerate((
        (bbx, bbo, 2), (bbx, bbo, 3), (bbo, bbo, 1), (bbo, bbx, 2), (bbo, bbx, 3), (bbx, bbx, 1)))]
    cp_zr.wait()
    bias_rows(lambda r: zr[x, pl.ds(r, 2)], bbx)
    for cpy in b_copies[:2]:
        cpy.start()
    cp_zo.wait()
    bias_rows(lambda r: zot[pl.ds(r, 2)], bbo)
    for cpy in b_copies[2:]:
        cpy.start()
    z_copies[0].start()

    for wdst, wsrc in ((wtsb, w_tsb), (wteb, w_teb)):
        wdst[0:4] = wsrc[...].astype(F32)
        wdst[4:E8] = jnp.zeros((4, N), F32)
    mk = mask_ref[x].astype(F32)
    mkb = mk.astype(BF16)
    ninv[...] = 1.0 / (mm(mkb, mkb, TN) + OPM_EPS)
    mtr[...] = jnp.transpose(mk)
    mcb[...] = (mk - 1.0) * (MASK_SCALE * LOG2E)
    mrb[1] = jnp.transpose(mcb[...])
    mrb[0] = jnp.transpose((mask_ref[ox].astype(F32) - 1.0) * (MASK_SCALE * LOG2E))
    res_bias = (res_ref[pl.ds(x, 1), :].astype(F32) - 1.0) * (MASK_SCALE * LOG2E)
    mrs[...] = jnp.transpose(jnp.broadcast_to(res_bias, (N, N)))
    def mask_tables(p, carry):
        mrow[p] = pltpu.roll(mrb[p // T16], (N - dev * B - 2 * (p % T16)) % N, 1)
        mcol[p] = pltpu.roll(mcb[...], (N - (2 * (p // T16) + c) * B - 2 * (p % T16)) % N, 1)
        return carry
    lax.fori_loop(0, B, mask_tables, 0)
    for e in range(B):
        ctf[pl.ds(e * COL_PITCH, B)] = w_oo[B * e:B * e + B].astype(F32)
    def perm_oo(f, carry):
        xf0[rows_at(B * f, B)] = ctf[pl.ds(f, B, stride=COL_PITCH), :]
        return carry
    lax.fori_loop(0, B, perm_oo, 0)
    for t in range(E8):
        woot[:, N * t:N * t + N] = jnp.transpose(xf0[N * t:N * t + N, :]).astype(BF16)

    def bias_table(n, src):
        for cpy in b_copies[3 * n:3 * n + 3]:
            cpy.wait_recv()
        bbf[...] = src[...].astype(F32) * LOG2E
        for h in range(E8):
            bt[n, h] = jnp.transpose(bbf[pl.ds(h, N, stride=E8), :])
    bias_table(0, bbo)

    cp_mo.wait()
    cp_mx.wait()

    def xa_copy(q, t, rel):
        rows = rows_at(t * E8, E8)
        return remote(rst.at[rel, rows, q], xx.at[1 + rel, rows, q], xa_s.at[q, t, rel], xa_r.at[q, t, rel], 2 + rel)

    def xb_copy(t):
        return remote(rst.at[1, rows_at(B + t * E8, E8)], xx.at[0, rows_at(t * E8, E8)], xb_s.at[t], xb_r.at[t], 1)

    def row_x(p):
        return ms[jnp.where(p < T16, ox, x), pl.ds(2 * (p % T16), 2)].reshape(W, W).astype(F32)

    def lane_mask(ref, p, u):
        return jnp.broadcast_to(ref[p][:, u:u + 1], (N, N))

    def row_emit(p, slot, new):
        new = new.reshape(2, 2, 2, B, W)
        even, odd = new[:, :, 0], new[:, :, 1]
        rst[0, pl.ds(2 * p, 2)] = jnp.where(c == 0, even, odd).astype(BF16)
        rst[1, pl.ds(2 * p, 2)] = jnp.where(c == 0, odd, even).astype(BF16)

    def row_four(t, carry):
        @pl.when(t == 3)
        def _():
            bias_table(1, bbx)

        def bias_at(p):
            return lambda h: bt[jnp.minimum(p + 1, 31) // T16, h]

        for e in range(4):
            row = Attention(st, w_row, w_row_o, E8, row_x, bias_at(4 * t + e),
                            lambda p, u: lane_mask(mrow, p, u), row_emit)
            row.step(4 * t + e, e, 31)

        @pl.when(jnp.logical_and(t > 0, t < 5))
        def _():
            for rel in range(2):
                xa_copy(0, t - 1, rel).start()

        @pl.when(t == 4)
        def _():
            for tt in range(4):
                for rel in range(2):
                    xa_copy(1, tt, rel).start()
            z_copies[1].start()

        @pl.when(t > 4)
        def _():
            xb_copy(t - 5).start()
        return carry
    row = Attention(st, w_row, w_row_o, E8, row_x, lambda h: bt[0, h], lambda p, u: lane_mask(mrow, p, u), row_emit)
    row.begin()
    lax.fori_loop(0, E8, row_four, 0)
    row.end(31)
    xb_copy(3).start()
    for t in range(4):
        xb_copy(t).wait_recv()

    def mo_copies(q):
        out = []
        res0 = pl.multiple_of((2 * q + c) * B, B)
        for flip in range(4):
            src = mo.at[pl.ds(peer(flip) * B, B), q]
            dst = m_out.at[x, :, pl.ds(res0, B)]
            if flip == 0:
                out.append(pltpu.make_async_copy(src, dst, mo_l.at[q]))
            else:
                out.append(remote(src, dst, mo_s.at[q, flip - 1], mo_r.at[q, flip - 1], flip))
        return out

    def c_copy(q):
        rows = rows_at((2 * q + c) * K1, K1)
        return remote(ctx.at[rows], ctx.at[rows], c_s.at[q], c_r.at[q], 1)

    def col_x(p):
        return jnp.concatenate([
            jnp.concatenate([ref[pl.ds(2 * p + u, N, stride=COL_PITCH), :] for ref in (xf0, xf1)], axis=1)
            for u in range(2)], axis=0)

    def col_chunk(q, carry):
        for t in range(4):
            for rel in range(2):
                xa_copy(q, t, rel).wait_recv()
        for flip in range(4):
            base = peer(flip) * (B * COL_PITCH)
            for r in range(B):
                v = (xx[flip - 1, r, q] if flip else rst[0, B + r, q]).astype(F32)
                rows = pl.ds(pl.multiple_of(base + r * COL_PITCH, E8), B)
                xf0[rows] = v[:, :N]
                xf1[rows] = v[:, N:]

        def col_post(p, slot):
            ac = mm(w_ac[...], layer_norm(nw[slot].astype(F32)), NT).astype(BF16).astype(F32)
            for u in range(2):
                loc = q * B + 2 * p + u
                nat = (2 * q + c) * B + 2 * p + u
                acm = (ac[:, N * u:N * u + N] * mtr[pl.ds(nat, 1), :]).astype(BF16)
                at[rows_at(loc * B, B)] = acm[0:B]
                ctx[rows_at(nat * B, B)] = acm[B:2 * B]

        def col_emit(p, slot, new):
            nw[slot] = new.astype(BF16)
            for u in range(2):
                of0[pl.ds(2 * p + u, N, stride=COL_PITCH), :] = new[N * u:N * u + N, :N]
                of1[pl.ds(2 * p + u, N, stride=COL_PITCH), :] = new[N * u:N * u + N, N:]

        col = Attention(st, w_col, w_col_o, E8, col_x, lambda h: None,
                        lambda p, u: lane_mask(mcol, q * T16 + p, u), col_emit, col_post)

        def col_four(t, carry2):
            for e in range(4):
                col.step(4 * t + e, e, 15)
            return carry2
        col.begin()
        lax.fori_loop(0, 4, col_four, 0)
        col.end(15)
        for r in range(N):
            rows = pl.ds(r * COL_PITCH, B)
            mo[r, q] = jnp.concatenate([of0[rows, :], of1[rows, :]], axis=1).astype(BF16)
        c_copy(q).start()
        for cpy in mo_copies(q):
            cpy.start()
        return carry
    lax.fori_loop(0, 2, col_chunk, 0)

    for q in range(2):
        c_copy(q).wait_recv()
    for j in range(N):
        ctf[pl.ds(j * COL_PITCH, B)] = ctx[B * j:B * j + B].astype(F32)

    def perm_c(f, carry):
        cp[rows_at(f * N, N)] = ctf[pl.ds(f, N, stride=COL_PITCH), :].astype(BF16)
        return carry
    lax.fori_loop(0, B, perm_c, 0)
    for cpy in z_copies:
        cpy.wait_recv()

    def opm_place(ib):
        k, r0 = ib // 4, (ib % 4) * E8
        return k, r0, (2 * k + c) * B + r0

    def opm_outer(ib, slot, fp):
        nat0 = opm_place(ib)[2]
        o = mm(at[rows_at(ib * W, W)], cp[fp * W:fp * W + W], NT)
        for i in range(E8):
            nrow = ninv[pl.ds(nat0 + i, 1), :]
            for ff in range(2):
                blk = o[B * i:B * i + B, N * ff:N * ff + N] * nrow
                rr[slot, i, fp * 64 + B * ff:fp * 64 + B * ff + B] = blk.astype(BF16)

    def pair_place(p):
        return p // T16, 2 * (p % T16)

    def opm_product(slot, ip, us):
        ut[us] = mm(woot[...], jnp.concatenate([rr[slot, 2 * ip], rr[slot, 2 * ip + 1]], axis=1), NN)

    def opm_update(p, us):
        k, r = pair_place(p)
        upd = jnp.concatenate([jnp.transpose(ut[us, :, :N]), jnp.transpose(ut[us, :, N:])], axis=0)
        zn = (zr[k, pl.ds(r, 2)].reshape(W, N).astype(F32) + upd).astype(BF16)
        nw[us, :, 0:N] = zn
        ms[k, pl.ds(r, 2), :, 0:N] = zn.reshape(2, N, N)

    def opm_bias(p, us):
        k, r = pair_place(p)
        b = mm(wtsb[...].astype(BF16), layer_norm(nw[us, :, 0:N].astype(F32)), NT)
        bs[rows_at(((2 * k + c) * B + r) * E8, T16)] = side_by_side(b).astype(BF16).astype(F32)

    def opm_two(t, carry):
        for e in range(E8):
            p = E8 * t + e
            slot = e // 4
            opm_bias(jnp.maximum(p - 2, 0), e % 2)
            opm_update(jnp.maximum(p - 1, 0), 1 - e % 2)
            nxt = jnp.minimum(2 * t + slot + 1, 7)
            for f in range(4):
                opm_outer(nxt, 1 - slot, e % 4 * 4 + f)
            opm_product(slot, e % 4, e % 2)
        return carry
    for fp in range(T16):
        opm_outer(0, 0, fp)
    lax.fori_loop(0, 4, opm_two, 0)
    opm_update(31, 1)
    opm_bias(30, 0)
    opm_bias(31, 1)

    def tri_bias_copies(ref, s_sem, r_sem):
        out = []
        for k in range(2):
            rows = rows_at((2 * k + c) * W, W)
            out.append(remote(ref.at[rows], ref.at[rows], s_sem.at[k], r_sem.at[k], 1))
        return out
    bs_copies = tri_bias_copies(bs, bs_s, bs_r)
    for cpy in bs_copies:
        cpy.start()
    for cpy in bs_copies:
        cpy.wait_recv()
    mres = mrs[...]
    for h in range(4):
        bts[h] = jnp.transpose(bs[pl.ds(h, N, stride=E8), :]) * LOG2E + mres

    def zx_copy(ob):
        rows = rows_at(ob * E8, E8)
        return remote(zs.at[rows], zx.at[c, rows], zx_s.at[ob], zx_r.at[ob], 1)

    def ts_x(p):
        return ms[p // T16, pl.ds(2 * (p % T16), 2), :, 0:N].reshape(W, N).astype(F32)

    def ts_post(p, slot):
        b = mm(wteb[...].astype(BF16), layer_norm(nw[slot, :, 0:N].astype(F32)), NT)
        nat = (2 * (p // T16) + c) * B + 2 * (p % T16)
        be[rows_at(nat * E8, T16)] = side_by_side(b).astype(BF16).astype(F32)

    def ts_emit(p, slot, new):
        nw[slot, :, 0:N] = new.astype(BF16)
        new = new.reshape(2, 2, 2, B, N)
        even, odd = new[:, :, 0], new[:, :, 1]
        zx[c, pl.ds(2 * p, 2)] = jnp.where(c == 0, even, odd).astype(BF16)
        zs[pl.ds(2 * p, 2)] = jnp.where(c == 0, odd, even).astype(BF16)

    ts = Attention(st, w_ts, w_ts_o, 4, ts_x, lambda h: bts[h], lambda p, u: None, ts_emit, ts_post)

    def ts_four(ob, carry):
        for e in range(4):
            ts.step(4 * ob + e, e, 31)

        @pl.when(ob > 0)
        def _():
            zx_copy(ob - 1).start()
        return carry
    ts.begin()
    lax.fori_loop(0, E8, ts_four, 0)
    ts.end(31)
    zx_copy(7).start()
    be_copies = tri_bias_copies(be, be_s, be_r)
    for cpy in be_copies:
        cpy.start()
    for cpy in be_copies:
        cpy.wait_recv()
    for h in range(4):
        bte[h] = be[pl.ds(h, N, stride=E8), :] * LOG2E + mres

    def zx_wait(ob, carry):
        zx_copy(ob).wait_recv()
        return carry
    lax.fori_loop(0, E8, zx_wait, 0)

    def zo_copies(ci, q, hf):
        out = []
        col0 = pl.multiple_of((2 * q + c) * B + hf * T16, T16)
        h16 = pl.multiple_of(hf * T16, T16)
        for flip in range(4):
            home = peer(flip)
            src = zo.at[pl.ds(home * B, B), q, pl.ds(h16, T16)]
            dst = z_out.at[x, :, pl.ds(col0, T16)]
            if flip == 0:
                out.append(pltpu.make_async_copy(src, dst, zo_l.at[ci]))
            else:
                out.append(remote(src, dst, zo_s.at[ci, flip - 1], zo_r.at[ci, flip - 1], flip))
        return out

    def te_chunk(ci, carry):
        q = ci // 2
        hf = ci % 2
        h16 = pl.multiple_of(hf * T16, T16)
        for c2 in range(2):
            for k in range(2):
                for r in range(B):
                    rows = pl.ds(((2 * k + c2) * B + r) * TRI_PITCH, T16)
                    zf[rows] = zx[c2, k * B + r, q, pl.ds(h16, T16), :].astype(F32)

        def te_x(p):
            return jnp.concatenate([zf[pl.ds(2 * p + u, N, stride=TRI_PITCH), :] for u in range(2)], axis=0)

        def te_emit(p, slot, new):
            for u in range(2):
                zof[pl.ds(2 * p + u, N, stride=TRI_PITCH), :] = new[N * u:N * u + N]

        te = Attention(st, w_te, w_te_o, 4, te_x, lambda h: bte[h], lambda p, u: None, te_emit)

        def te_four(t, carry2):
            for e in range(4):
                te.step(4 * t + e, e, 7)
            return carry2
        te.begin()
        lax.fori_loop(0, 2, te_four, 0)
        te.end(7)
        for r in range(N):
            zo[r, q, pl.ds(h16, T16), :] = zof[pl.ds(r * TRI_PITCH, T16), :].astype(BF16)
        for cpy in zo_copies(ci, q, hf):
            cpy.start()
        return carry
    lax.fori_loop(0, 4, te_chunk, 0)

    for cpy in b_copies + bs_copies + be_copies + z_copies:
        cpy.wait_send()
    def drain8(j, carry):
        zx_copy(j).wait_send()
        return carry
    lax.fori_loop(0, E8, drain8, 0)
    for t in range(4):
        xb_copy(t).wait_send()
        for rel in range(2):
            xa_copy(0, t, rel).wait_send()
            xa_copy(1, t, rel).wait_send()
    for q in range(2):
        c_copy(q).wait_send()
        for cpy in mo_copies(q):
            cpy.wait()
    def drain4(ci, carry):
        for cpy in zo_copies(ci, ci // 2, ci % 2):
            cpy.wait()
        return carry
    lax.fori_loop(0, 4, drain4, 0)


def finish(m_ref, z_ref, m_out, z_out, m_buf, z_buf, in_sem, out_sem):
    steps = []
    for n in range(E8):
        for src, buf, dst, k in ((m_ref, m_buf, m_out, 0), (z_ref, z_buf, z_out, 1)):
            at = (n // 4, pl.ds(n % 4 * E8, E8))
            steps.append((pltpu.make_async_copy(src.at[at], buf.at[at], in_sem.at[k, n]),
                          pltpu.make_async_copy(buf.at[at], dst.at[at], out_sem.at[k, n])))
    for load, _ in steps:
        load.start()
    for load, store in steps:
        load.wait()
        store.start()
    for _, store in steps:
        store.wait()


def weight_t(w):
    return w.reshape(w.shape[0], -1).T


def solution(mesh):
    rows_spec = P(PART_AXIS, GROUP_AXIS, None, None)
    in_specs = (rows_spec, rows_spec, P(PART_AXIS, None, None), P(PART_AXIS, None)) + (P(),) * 13

    def block(m, z, mask, res_mask, *weights):
        (w_row_bias, w_row_qkvg, w_row_out, w_col_qkvg, w_col_out, w_opm_ac, w_opm_out,
         w_ts_bias, w_ts_qkvg, w_ts_out, w_te_bias, w_te_qkvg, w_te_out) = weights
        args = (m, z, mask, res_mask, w_row_bias.T, w_ts_bias.T, w_te_bias.T,
                weight_t(w_row_qkvg), w_row_out.reshape(W, W), weight_t(w_col_qkvg), w_col_out.reshape(W, W),
                weight_t(w_opm_ac), w_opm_out.reshape(K1, N),
                weight_t(w_ts_qkvg), w_ts_out.reshape(N, N), weight_t(w_te_qkvg), w_te_out.reshape(N, N))
        vm = pl.BlockSpec(memory_space=pltpu.VMEM)
        hbm = pl.BlockSpec(memory_space=pl.ANY)
        V = pltpu.VMEM
        row_z, row_m, sq = (B, N, N), (B, N, W), (N, N)
        scratch = [V(shape, BF16) for shape in (
            (2,) + row_z, row_z, (2,) + row_m, (3, B, 2, B, W), (2, 64, 2, B, W), (K1, N), (K1, N))]
        scratch += [V(shape, F32) for shape in (
            (K1, N), (2, E8) + sq) + ((N * COL_PITCH, N),) * 4]
        scratch += [V((N, 2, B, W), BF16), V((2048, N), BF16), V((B * N, N), BF16), V((N * COL_PITCH, N), F32),
                    V((B * N, N), BF16), V(sq, F32), V(sq, F32), V((N, K1), BF16), V((2, E8, K1, N), BF16)]
        scratch += [V(shape, F32) for shape in ((K1, N), (4,) + sq, (K1, N), (4,) + sq)]
        scratch += [V((2, 64, 2, B, N), BF16), V((64, 2, B, N), BF16),
                    V((N, 2, B, N), BF16)]
        scratch += [V((2, W, W), BF16)] * 2 + [V((4, W, W), BF16), V((4, W, W), F32), V((2, T16) + sq, F32),
                    V((2, T16, N), F32), V((2, W, W), BF16), V((2, W, W), BF16), V((2, W, W), BF16), V((E8, N), F32), V((E8, N), F32)]
        scratch += [V(sq, F32), V((2,) + sq, F32), V(sq, F32)] + [V((B,) + sq, F32)] * 2 + [V((2, N, W), F32)]
        S = pltpu.SemaphoreType.DMA
        scratch += [S(shape) for shape in (
            (4,), (2,), (2,), (6,), (6,), (2, 4, 2), (2, 4, 2), (4,), (4,), (2, 3), (2, 3), (2,), (2,), (2,),
            (2,), (2,), (2,), (2,), (E8,), (E8,), (4, 3), (4, 3), (4,))]
        outs = pl.pallas_call(
            mega,
            out_shape=(jax.ShapeDtypeStruct(m.shape, BF16), jax.ShapeDtypeStruct(z.shape, BF16)),
            in_specs=[hbm, hbm] + [vm] * 15,
            out_specs=(hbm, hbm),
            scratch_shapes=scratch,
            compiler_params=pltpu.CompilerParams(collective_id=0, has_side_effects=True,
                                                 vmem_limit_bytes=62 << 20),
            name='evoformer_block',
        )(*args)
        return pl.pallas_call(
            finish,
            out_shape=(jax.ShapeDtypeStruct(m.shape, BF16), jax.ShapeDtypeStruct(z.shape, BF16)),
            in_specs=[hbm, hbm],
            out_specs=(hbm, hbm),
            scratch_shapes=[V(m.shape, BF16), V(z.shape, BF16), S((2, E8)), S((2, E8))],
            name='finish',
        )(*outs)

    return jax.shard_map(block, mesh=mesh, in_specs=in_specs, out_specs=(rows_spec, rows_spec), check_vma=False)
```

```python
import functools

import jax
import jax.numpy as jnp
from jax import lax
from jax.experimental import pallas as pl
from jax.experimental.pallas import tpu as pltpu
from jax.sharding import PartitionSpec as P

F32 = jnp.float32
BF16 = jnp.bfloat16
MASK_SCALE = 10000.0
LN_EPS = 1e-5
OPM_EPS = 1e-3
LOG2E = 1.4426950408889634
HEAD_DIM = 32
N = 128
B = 32
W = 256
K1 = 1024
T16 = 16
E8 = 8
COL_PITCH = 40
TRI_PITCH = 24
SCALE2 = (HEAD_DIM ** -0.5) * LOG2E
PART_AXIS = 'data'
GROUP_AXIS = 'dap'
MESH_ID = pl.DeviceIdType.MESH
NT = (((1,), (1,)), ((), ()))
NN = (((1,), (0,)), ((), ()))
TN = (((0,), (0,)), ((), ()))


def mm(lhs, rhs, dims):
    return lax.dot_general(lhs, rhs, dims, preferred_element_type=F32)


def layer_norm(xf):
    mean = jnp.mean(xf, axis=-1, keepdims=True)
    cen = xf - mean
    var = jnp.mean(cen * cen, axis=-1, keepdims=True)
    return (cen * lax.rsqrt(var + LN_EPS)).astype(BF16)


class Attention:
    def __init__(self, st, wt_ref, wo_ref, n_heads, load_x, bias_of, mask_of, emit, post=None):
        self.qs, self.ks, self.vs, self.gs, self.lg, self.mx, self.os, self.ys = st
        self.wt, self.wo, self.n_heads, self.hd = wt_ref, wo_ref, n_heads, n_heads * HEAD_DIM
        self.load_x, self.bias_of, self.mask_of, self.emit, self.post = load_x, bias_of, mask_of, emit, post
        self.items = [(u, h) for u in range(2) for h in range(0, n_heads, 2)]

    def n_parts(self, p, i):
        xf = self.load_x(p)
        for b in range(4):
            rows = slice(64 * b, 64 * b + 64)
            self.ys[i % 2, rows, 0:xf.shape[1]] = layer_norm(xf[rows])
            yield

    def p_part(self, i, part):
        hd = self.hd
        y = self.ys[i % 2, :, 0:self.wt.shape[1]]
        w = self.wt[part * hd:(part + 1) * hd]
        if part == 0:
            self.qs[i % 2, 0:hd] = mm(w, y, NT).astype(BF16)
        elif part == 1:
            self.ks[i % 2, :, 0:hd] = mm(y, w, NT).astype(BF16)
        elif part == 2:
            self.vs[i % 4, 0:hd] = mm(w, y, NT).astype(BF16)
        else:
            self.gs[i % 4, 0:hd] = jax.nn.sigmoid(mm(w, y, NT))

    def l_part(self, p, i, item):
        u, h = item
        tok = slice(N * u, N * u + N)
        blocks = []
        for hh in (h, h + 1):
            h4 = hh % 4
            rows = [self.qs[i % 2, B * hh:B * hh + B, tok]]
            if h4 > 0:
                rows.insert(0, jnp.zeros((B * h4, N), BF16))
            if h4 < 3:
                rows.append(jnp.zeros((N - B - B * h4, N), BF16))
            blocks.append(jnp.concatenate(rows, axis=0))
        g0 = h // 4 * N
        logits = mm(self.ks[i % 2, tok, g0:g0 + N], jnp.concatenate(blocks, axis=1), NN)
        mask_col = self.mask_of(p, u)
        for n, hh in enumerate((h, h + 1)):
            lg = logits[:, N * n:N * n + N] * SCALE2
            bias = self.bias_of(hh)
            if bias is not None:
                lg = lg + bias
            if mask_col is not None:
                lg = lg + mask_col
            row = u * self.n_heads + hh
            self.lg[i % 2, row] = lg
            self.mx[i % 2, row:row + 1] = jnp.max(lg, axis=0, keepdims=True)

    def s_part(self, i, item):
        u, h = item
        tok = slice(N * u, N * u + N)
        ps, inv = [], []
        for hh in (h, h + 1):
            row = u * self.n_heads + hh
            ex = jnp.exp2(self.lg[i % 2, row] - self.mx[i % 2, row:row + 1])
            inv.append(1.0 / jnp.sum(ex, axis=0, keepdims=True))
            ps.append(ex.astype(BF16))
        h0 = h * B
        ov = mm(self.vs[i % 4, h0:h0 + 2 * B, tok], jnp.concatenate(ps, axis=1), NN)
        o = jnp.concatenate([ov[0:B, 0:N] * inv[0], ov[B:2 * B, N:W] * inv[1]], axis=0)
        self.os[i % 2, h0:h0 + 2 * B, tok] = (o * self.gs[i % 4, h0:h0 + 2 * B, tok]).astype(BF16)

    def o_part(self, p, i):
        self.emit(p, i % 2, self.load_x(p) + mm(self.os[i % 2, 0:self.hd], self.wo[...], TN))

    def step(self, p, i, last):
        if self.post is not None:
            self.post(jnp.maximum(p - 2, 0), i % 2)
        self.o_part(jnp.maximum(p - 1, 0), i - 1)
        norm = self.n_parts(jnp.minimum(p + 3, last), i + 3)
        nxt = jnp.minimum(p + 1, last)
        for n, item in enumerate(self.items):
            self.l_part(nxt, i + 1, item)
            self.s_part(i, item)
            for part in range(4):
                if part * len(self.items) // 4 == n:
                    next(norm)
                    self.p_part(i + 2, part)

    def begin(self):
        for i in range(3):
            for _ in self.n_parts(i, i):
                pass
            for part in range(4 if i < 2 else 0):
                self.p_part(i, part)
        for item in self.items:
            self.l_part(0, 0, item)

    def end(self, last):
        self.o_part(last, 3)
        if self.post is not None:
            self.post(last - 1, 0)
            self.post(last, 1)


def rows_at(start, size):
    return pl.ds(pl.multiple_of(start, size), size)


def side_by_side(b):
    return jnp.concatenate([b[:, :N], b[:, N:]], axis=0)


def mega(m_in, z_in, mask_ref, res_ref, w_rb, w_tsb, w_teb, w_row, w_row_o, w_col, w_col_o, w_ac, w_oo,
         w_ts, w_ts_o, w_te, w_te_o, m_out, z_out,
         zr, zot, ms, xx, rst, bbx, bbo, bbf, bt, xf0, xf1, of0, of1, mo, at, ctx, ctf, cp, ninv, mtr, woot, rr,
         bs, bts, be, bte, zx, zs, zo, qs, ks, vs, gs, lgs, mxs, ots, ys, nw, wtsb, wteb, mcb, mrb, mrs, mrow, mcol, ut,
         l_sem, zi_s, zi_r, b_s, b_r, xa_s, xa_r, xb_s, xb_r, mo_s, mo_r, mo_l, c_s, c_r, bs_s, bs_r, be_s, be_r,
         zx_s, zx_r, zo_s, zo_r, zo_l):
    st = (qs, ks, vs, gs, lgs, mxs, ots, ys)
    zf, zof = xf1, of1
    dat = lax.axis_index(PART_AXIS)
    dev = lax.axis_index(GROUP_AXIS)
    x = dev // 2
    c = dev % 2
    ox = 1 - x

    def peer(flip):
        px = ox if flip >= 2 else x
        pc = (1 - c) if flip % 2 else c
        return px * 2 + pc

    def remote(src, dst, s_sem, r_sem, flip):
        return pltpu.make_async_remote_copy(src, dst, s_sem, r_sem, device_id=(dat, peer(flip)),
                                            device_id_type=MESH_ID)

    barrier = pltpu.get_barrier_semaphore()
    for flip in (1, 2, 3):
        pl.semaphore_signal(barrier, inc=1, device_id=(dat, peer(flip)), device_id_type=MESH_ID)
    cp_zo = pltpu.make_async_copy(z_in.at[ox], zot, l_sem.at[0])
    cp_zr = pltpu.make_async_copy(z_in.at[x], zr.at[x], l_sem.at[1])
    cp_mo = pltpu.make_async_copy(m_in.at[ox], ms.at[ox], l_sem.at[2])
    cp_mx = pltpu.make_async_copy(m_in.at[x], ms.at[x], l_sem.at[3])
    for cpy in (cp_zr, cp_zo, cp_mo, cp_mx):
        cpy.start()
    pl.semaphore_wait(barrier, 3)

    z_copies = []
    for n, (first, size) in enumerate(((0, 4), (4, E8), (12, 20))):
        rows = pl.ds(first, size)
        z_copies.append(remote(z_in.at[ox, rows], zr.at[x, rows], zi_s.at[n], zi_r.at[n], 2))
    z_copies[0].start()

    row0 = pl.multiple_of(dev * W, W)
    own = pl.ds(row0, W)

    def bias_rows(load, dst):
        def body(g, carry):
            for p in range(4):
                y = layer_norm(load(E8 * g + 2 * p).reshape(W, N).astype(F32))
                dst[rows_at(row0 + 64 * g + T16 * p, T16)] = side_by_side(mm(w_rb[...], y, NT)).astype(BF16)
            return carry
        lax.fori_loop(0, 4, body, 0)

    b_copies = [remote(src.at[own], dst.at[own], b_s.at[n], b_r.at[n], flip) for n, (src, dst, flip) in enumerate((
        (bbx, bbo, 2), (bbx, bbo, 3), (bbo, bbo, 1), (bbo, bbx, 2), (bbo, bbx, 3), (bbx, bbx, 1)))]
    cp_zr.wait()
    bias_rows(lambda r: zr[x, pl.ds(r, 2)], bbx)
    for cpy in b_copies[:2]:
        cpy.start()
    cp_zo.wait()
    bias_rows(lambda r: zot[pl.ds(r, 2)], bbo)
    for cpy in b_copies[2:]:
        cpy.start()
    z_copies[1].start()

    for wdst, wsrc in ((wtsb, w_tsb), (wteb, w_teb)):
        wdst[0:4] = wsrc[...].astype(F32)
        wdst[4:E8] = jnp.zeros((4, N), F32)
    mk = mask_ref[x].astype(F32)
    mkb = mk.astype(BF16)
    ninv[...] = 1.0 / (mm(mkb, mkb, TN) + OPM_EPS)
    mtr[...] = jnp.transpose(mk)
    mcb[...] = (mk - 1.0) * (MASK_SCALE * LOG2E)
    mrb[1] = jnp.transpose(mcb[...])
    mrb[0] = jnp.transpose((mask_ref[ox].astype(F32) - 1.0) * (MASK_SCALE * LOG2E))
    res_bias = (res_ref[pl.ds(x, 1), :].astype(F32) - 1.0) * (MASK_SCALE * LOG2E)
    mrs[...] = jnp.transpose(jnp.broadcast_to(res_bias, (N, N)))
    def mask_tables(p, carry):
        mrow[p] = pltpu.roll(mrb[p // T16], (N - dev * B - 2 * (p % T16)) % N, 1)
        mcol[p] = pltpu.roll(mcb[...], (N - (2 * (p // T16) + c) * B - 2 * (p % T16)) % N, 1)
        return carry
    lax.fori_loop(0, B, mask_tables, 0)
    for e in range(B):
        ctf[pl.ds(e * COL_PITCH, B)] = w_oo[B * e:B * e + B].astype(F32)
    def perm_oo(f, carry):
        xf0[rows_at(B * f, B)] = ctf[pl.ds(f, B, stride=COL_PITCH), :]
        return carry
    lax.fori_loop(0, B, perm_oo, 0)
    for t in range(E8):
        woot[:, N * t:N * t + N] = jnp.transpose(xf0[N * t:N * t + N, :]).astype(BF16)

    def bias_table(n, src):
        for cpy in b_copies[3 * n:3 * n + 3]:
            cpy.wait_recv()
        bbf[...] = src[...].astype(F32) * LOG2E
        for h in range(E8):
            bt[n, h] = jnp.transpose(bbf[pl.ds(h, N, stride=E8), :])
    bias_table(0, bbo)

    cp_mo.wait()
    cp_mx.wait()

    def xa_copy(q, t, rel):
        rows = rows_at(t * E8, E8)
        return remote(rst.at[rel, rows, q], xx.at[1 + rel, rows, q], xa_s.at[q, t, rel], xa_r.at[q, t, rel], 2 + rel)

    def xb_copy(t):
        return remote(rst.at[1, rows_at(B + t * E8, E8)], xx.at[0, rows_at(t * E8, E8)], xb_s.at[t], xb_r.at[t], 1)

    def row_x(p):
        return ms[jnp.where(p < T16, ox, x), pl.ds(2 * (p % T16), 2)].reshape(W, W).astype(F32)

    def lane_mask(ref, p, u):
        return jnp.broadcast_to(ref[p][:, u:u + 1], (N, N))

    def row_emit(p, slot, new):
        new = new.reshape(2, 2, 2, B, W)
        even, odd = new[:, :, 0], new[:, :, 1]
        rst[0, pl.ds(2 * p, 2)] = jnp.where(c == 0, even, odd).astype(BF16)
        rst[1, pl.ds(2 * p, 2)] = jnp.where(c == 0, odd, even).astype(BF16)

    def row_four(t, carry):
        @pl.when(t == 3)
        def _():
            bias_table(1, bbx)

        def bias_at(p):
            return lambda h: bt[jnp.minimum(p + 1, 31) // T16, h]

        for e in range(4):
            row = Attention(st, w_row, w_row_o, E8, row_x, bias_at(4 * t + e),
                            lambda p, u: lane_mask(mrow, p, u), row_emit)
            row.step(4 * t + e, e, 31)

        @pl.when(jnp.logical_and(t > 0, t < 5))
        def _():
            for rel in range(2):
                xa_copy(0, t - 1, rel).start()

        @pl.when(t == 4)
        def _():
            for tt in range(4):
                for rel in range(2):
                    xa_copy(1, tt, rel).start()
            z_copies[2].start()

        @pl.when(t > 4)
        def _():
            xb_copy(t - 5).start()
        return carry
    row = Attention(st, w_row, w_row_o, E8, row_x, lambda h: bt[0, h], lambda p, u: lane_mask(mrow, p, u), row_emit)
    row.begin()
    lax.fori_loop(0, E8, row_four, 0)
    row.end(31)
    xb_copy(3).start()
    for t in range(4):
        xb_copy(t).wait_recv()

    def mo_copies(q):
        out = []
        res0 = pl.multiple_of((2 * q + c) * B, B)
        for flip in range(4):
            src = mo.at[pl.ds(peer(flip) * B, B), q]
            dst = m_out.at[x, :, pl.ds(res0, B)]
            if flip == 0:
                out.append(pltpu.make_async_copy(src, dst, mo_l.at[q]))
            else:
                out.append(remote(src, dst, mo_s.at[q, flip - 1], mo_r.at[q, flip - 1], flip))
        return out

    def c_copy(q):
        rows = rows_at((2 * q + c) * K1, K1)
        return remote(ctx.at[rows], ctx.at[rows], c_s.at[q], c_r.at[q], 1)

    def col_x(p):
        return jnp.concatenate([
            jnp.concatenate([ref[pl.ds(2 * p + u, N, stride=COL_PITCH), :] for ref in (xf0, xf1)], axis=1)
            for u in range(2)], axis=0)

    def col_chunk(q, carry):
        for t in range(4):
            for rel in range(2):
                xa_copy(q, t, rel).wait_recv()
        for flip in range(4):
            base = peer(flip) * (B * COL_PITCH)
            for r in range(B):
                v = (xx[flip - 1, r, q] if flip else rst[0, B + r, q]).astype(F32)
                rows = pl.ds(pl.multiple_of(base + r * COL_PITCH, E8), B)
                xf0[rows] = v[:, :N]
                xf1[rows] = v[:, N:]

        def col_post(p, slot):
            ac = mm(w_ac[...], layer_norm(nw[slot].astype(F32)), NT).astype(BF16).astype(F32)
            for u in range(2):
                loc = q * B + 2 * p + u
                nat = (2 * q + c) * B + 2 * p + u
                acm = (ac[:, N * u:N * u + N] * mtr[pl.ds(nat, 1), :]).astype(BF16)
                at[rows_at(loc * B, B)] = acm[0:B]
                ctx[rows_at(nat * B, B)] = acm[B:2 * B]

        def col_emit(p, slot, new):
            nw[slot] = new.astype(BF16)
            for u in range(2):
                of0[pl.ds(2 * p + u, N, stride=COL_PITCH), :] = new[N * u:N * u + N, :N]
                of1[pl.ds(2 * p + u, N, stride=COL_PITCH), :] = new[N * u:N * u + N, N:]

        col = Attention(st, w_col, w_col_o, E8, col_x, lambda h: None,
                        lambda p, u: lane_mask(mcol, q * T16 + p, u), col_emit, col_post)

        def col_four(t, carry2):
            for e in range(4):
                col.step(4 * t + e, e, 15)
            return carry2
        col.begin()
        lax.fori_loop(0, 4, col_four, 0)
        col.end(15)
        for r in range(N):
            rows = pl.ds(r * COL_PITCH, B)
            mo[r, q] = jnp.concatenate([of0[rows, :], of1[rows, :]], axis=1).astype(BF16)
        c_copy(q).start()
        for cpy in mo_copies(q):
            cpy.start()
        return carry
    lax.fori_loop(0, 2, col_chunk, 0)

    for q in range(2):
        c_copy(q).wait_recv()
    for j in range(N):
        ctf[pl.ds(j * COL_PITCH, B)] = ctx[B * j:B * j + B].astype(F32)

    def perm_c(f, carry):
        cp[rows_at(f * N, N)] = ctf[pl.ds(f, N, stride=COL_PITCH), :].astype(BF16)
        return carry
    lax.fori_loop(0, B, perm_c, 0)

    def opm_place(ib):
        k, r0 = jnp.where(ib < 4, x, ox), (ib % 4) * E8
        return k, r0, (2 * k + c) * B + r0

    def opm_outer(ib, slot, fp):
        k, r0, nat0 = opm_place(ib)
        o = mm(at[rows_at((k * B + r0) * B, W)], cp[fp * W:fp * W + W], NT)
        for i in range(E8):
            nrow = ninv[pl.ds(nat0 + i, 1), :]
            for ff in range(2):
                blk = o[B * i:B * i + B, N * ff:N * ff + N] * nrow
                rr[slot, i, fp * 64 + B * ff:fp * 64 + B * ff + B] = blk.astype(BF16)

    def pair_place(p):
        return jnp.where(p < T16, x, ox), 2 * (p % T16)

    def opm_product(slot, ip, us):
        ut[us] = mm(woot[...], jnp.concatenate([rr[slot, 2 * ip], rr[slot, 2 * ip + 1]], axis=1), NN)

    def opm_update(p, us):
        k, r = pair_place(p)
        upd = jnp.concatenate([jnp.transpose(ut[us, :, :N]), jnp.transpose(ut[us, :, N:])], axis=0)
        zn = (zr[k, pl.ds(r, 2)].reshape(W, N).astype(F32) + upd).astype(BF16)
        nw[us, :, 0:N] = zn
        ms[k, pl.ds(r, 2), :, 0:N] = zn.reshape(2, N, N)

    def opm_bias(p, us):
        k, r = pair_place(p)
        b = mm(wtsb[...].astype(BF16), layer_norm(nw[us, :, 0:N].astype(F32)), NT)
        bs[rows_at(((2 * k + c) * B + r) * E8, T16)] = side_by_side(b).astype(BF16).astype(F32)

    def opm_two(t, carry):
        @pl.when(t == 2)
        def _():
            for cpy in z_copies:
                cpy.wait_recv()

        for e in range(E8):
            p = E8 * t + e
            slot = e // 4
            opm_bias(jnp.maximum(p - 2, 0), e % 2)
            opm_update(jnp.maximum(p - 1, 0), 1 - e % 2)
            nxt = jnp.minimum(2 * t + slot + 1, 7)
            for f in range(4):
                opm_outer(nxt, 1 - slot, e % 4 * 4 + f)
            opm_product(slot, e % 4, e % 2)
        return carry
    for fp in range(T16):
        opm_outer(0, 0, fp)
    lax.fori_loop(0, 4, opm_two, 0)
    opm_update(31, 1)
    opm_bias(30, 0)
    opm_bias(31, 1)

    def tri_bias_copies(ref, s_sem, r_sem):
        out = []
        for k in range(2):
            rows = rows_at((2 * k + c) * W, W)
            out.append(remote(ref.at[rows], ref.at[rows], s_sem.at[k], r_sem.at[k], 1))
        return out
    bs_copies = tri_bias_copies(bs, bs_s, bs_r)
    for cpy in bs_copies:
        cpy.start()
    for cpy in bs_copies:
        cpy.wait_recv()
    mres = mrs[...]
    for h in range(4):
        bts[h] = jnp.transpose(bs[pl.ds(h, N, stride=E8), :]) * LOG2E + mres

    def zx_copy(ob):
        rows = rows_at(ob * E8, E8)
        return remote(zs.at[rows], zx.at[c, rows], zx_s.at[ob], zx_r.at[ob], 1)

    def ts_x(p):
        return ms[p // T16, pl.ds(2 * (p % T16), 2), :, 0:N].reshape(W, N).astype(F32)

    def ts_post(p, slot):
        b = mm(wteb[...].astype(BF16), layer_norm(nw[slot, :, 0:N].astype(F32)), NT)
        nat = (2 * (p // T16) + c) * B + 2 * (p % T16)
        be[rows_at(nat * E8, T16)] = side_by_side(b).astype(BF16).astype(F32)

    def ts_emit(p, slot, new):
        nw[slot, :, 0:N] = new.astype(BF16)
        new = new.reshape(2, 2, 2, B, N)
        even, odd = new[:, :, 0], new[:, :, 1]
        zx[c, pl.ds(2 * p, 2)] = jnp.where(c == 0, even, odd).astype(BF16)
        zs[pl.ds(2 * p, 2)] = jnp.where(c == 0, odd, even).astype(BF16)

    ts = Attention(st, w_ts, w_ts_o, 4, ts_x, lambda h: bts[h], lambda p, u: None, ts_emit, ts_post)

    def ts_four(ob, carry):
        for e in range(4):
            ts.step(4 * ob + e, e, 31)

        @pl.when(ob > 0)
        def _():
            zx_copy(ob - 1).start()
        return carry
    ts.begin()
    lax.fori_loop(0, E8, ts_four, 0)
    ts.end(31)
    zx_copy(7).start()
    be_copies = tri_bias_copies(be, be_s, be_r)
    for cpy in be_copies:
        cpy.start()
    for cpy in be_copies:
        cpy.wait_recv()
    for h in range(4):
        bte[h] = be[pl.ds(h, N, stride=E8), :] * LOG2E + mres

    def zx_wait(ob, carry):
        zx_copy(ob).wait_recv()
        return carry
    lax.fori_loop(0, E8, zx_wait, 0)

    def zo_copies(ci, q, hf):
        out = []
        col0 = pl.multiple_of((2 * q + c) * B + hf * T16, T16)
        h16 = pl.multiple_of(hf * T16, T16)
        for flip in range(4):
            home = peer(flip)
            src = zo.at[pl.ds(home * B, B), q, pl.ds(h16, T16)]
            dst = z_out.at[x, :, pl.ds(col0, T16)]
            if flip == 0:
                out.append(pltpu.make_async_copy(src, dst, zo_l.at[ci]))
            else:
                out.append(remote(src, dst, zo_s.at[ci, flip - 1], zo_r.at[ci, flip - 1], flip))
        return out

    def te_chunk(ci, carry):
        q = ci // 2
        hf = ci % 2
        h16 = pl.multiple_of(hf * T16, T16)
        for c2 in range(2):
            for k in range(2):
                for r in range(B):
                    rows = pl.ds(((2 * k + c2) * B + r) * TRI_PITCH, T16)
                    zf[rows] = zx[c2, k * B + r, q, pl.ds(h16, T16), :].astype(F32)

        def te_x(p):
            return jnp.concatenate([zf[pl.ds(2 * p + u, N, stride=TRI_PITCH), :] for u in range(2)], axis=0)

        def te_emit(p, slot, new):
            for u in range(2):
                zof[pl.ds(2 * p + u, N, stride=TRI_PITCH), :] = new[N * u:N * u + N]

        te = Attention(st, w_te, w_te_o, 4, te_x, lambda h: bte[h], lambda p, u: None, te_emit)

        def te_four(t, carry2):
            for e in range(4):
                te.step(4 * t + e, e, 7)
            return carry2
        te.begin()
        lax.fori_loop(0, 2, te_four, 0)
        te.end(7)
        for r in range(N):
            zo[r, q, pl.ds(h16, T16), :] = zof[pl.ds(r * TRI_PITCH, T16), :].astype(BF16)
        for cpy in zo_copies(ci, q, hf):
            cpy.start()
        return carry
    lax.fori_loop(0, 4, te_chunk, 0)

    for cpy in b_copies + bs_copies + be_copies + z_copies:
        cpy.wait_send()
    def drain8(j, carry):
        zx_copy(j).wait_send()
        return carry
    lax.fori_loop(0, E8, drain8, 0)
    for t in range(4):
        xb_copy(t).wait_send()
        for rel in range(2):
            xa_copy(0, t, rel).wait_send()
            xa_copy(1, t, rel).wait_send()
    for q in range(2):
        c_copy(q).wait_send()
        for cpy in mo_copies(q):
            cpy.wait()
    def drain4(ci, carry):
        for cpy in zo_copies(ci, ci // 2, ci % 2):
            cpy.wait()
        return carry
    lax.fori_loop(0, 4, drain4, 0)


def finish(m_ref, z_ref, m_out, z_out, m_buf, z_buf, in_sem, out_sem):
    steps = []
    for n in range(E8):
        for src, buf, dst, k in ((m_ref, m_buf, m_out, 0), (z_ref, z_buf, z_out, 1)):
            at = (n // 4, pl.ds(n % 4 * E8, E8))
            steps.append((pltpu.make_async_copy(src.at[at], buf.at[at], in_sem.at[k, n]),
                          pltpu.make_async_copy(buf.at[at], dst.at[at], out_sem.at[k, n])))
    for load, _ in steps:
        load.start()
    for load, store in steps:
        load.wait()
        store.start()
    for _, store in steps:
        store.wait()


def weight_t(w):
    return w.reshape(w.shape[0], -1).T


def solution(mesh):
    rows_spec = P(PART_AXIS, GROUP_AXIS, None, None)
    in_specs = (rows_spec, rows_spec, P(PART_AXIS, None, None), P(PART_AXIS, None)) + (P(),) * 13

    def block(m, z, mask, res_mask, *weights):
        (w_row_bias, w_row_qkvg, w_row_out, w_col_qkvg, w_col_out, w_opm_ac, w_opm_out,
         w_ts_bias, w_ts_qkvg, w_ts_out, w_te_bias, w_te_qkvg, w_te_out) = weights
        args = (m, z, mask, res_mask, w_row_bias.T, w_ts_bias.T, w_te_bias.T,
                weight_t(w_row_qkvg), w_row_out.reshape(W, W), weight_t(w_col_qkvg), w_col_out.reshape(W, W),
                weight_t(w_opm_ac), w_opm_out.reshape(K1, N),
                weight_t(w_ts_qkvg), w_ts_out.reshape(N, N), weight_t(w_te_qkvg), w_te_out.reshape(N, N))
        vm = pl.BlockSpec(memory_space=pltpu.VMEM)
        hbm = pl.BlockSpec(memory_space=pl.ANY)
        V = pltpu.VMEM
        row_z, row_m, sq = (B, N, N), (B, N, W), (N, N)
        scratch = [V(shape, BF16) for shape in (
            (2,) + row_z, row_z, (2,) + row_m, (3, B, 2, B, W), (2, 64, 2, B, W), (K1, N), (K1, N))]
        scratch += [V(shape, F32) for shape in (
            (K1, N), (2, E8) + sq) + ((N * COL_PITCH, N),) * 4]
        scratch += [V((N, 2, B, W), BF16), V((2048, N), BF16), V((B * N, N), BF16), V((N * COL_PITCH, N), F32),
                    V((B * N, N), BF16), V(sq, F32), V(sq, F32), V((N, K1), BF16), V((2, E8, K1, N), BF16)]
        scratch += [V(shape, F32) for shape in ((K1, N), (4,) + sq, (K1, N), (4,) + sq)]
        scratch += [V((2, 64, 2, B, N), BF16), V((64, 2, B, N), BF16),
                    V((N, 2, B, N), BF16)]
        scratch += [V((2, W, W), BF16)] * 2 + [V((4, W, W), BF16), V((4, W, W), F32), V((2, T16) + sq, F32),
                    V((2, T16, N), F32), V((2, W, W), BF16), V((2, W, W), BF16), V((2, W, W), BF16), V((E8, N), F32), V((E8, N), F32)]
        scratch += [V(sq, F32), V((2,) + sq, F32), V(sq, F32)] + [V((B,) + sq, F32)] * 2 + [V((2, N, W), F32)]
        S = pltpu.SemaphoreType.DMA
        scratch += [S(shape) for shape in (
            (4,), (3,), (3,), (6,), (6,), (2, 4, 2), (2, 4, 2), (4,), (4,), (2, 3), (2, 3), (2,), (2,), (2,),
            (2,), (2,), (2,), (2,), (E8,), (E8,), (4, 3), (4, 3), (4,))]
        outs = pl.pallas_call(
            mega,
            out_shape=(jax.ShapeDtypeStruct(m.shape, BF16), jax.ShapeDtypeStruct(z.shape, BF16)),
            in_specs=[hbm, hbm] + [vm] * 15,
            out_specs=(hbm, hbm),
            scratch_shapes=scratch,
            compiler_params=pltpu.CompilerParams(collective_id=0, has_side_effects=True,
                                                 vmem_limit_bytes=62 << 20),
            name='evoformer_block',
        )(*args)
        return pl.pallas_call(
            finish,
            out_shape=(jax.ShapeDtypeStruct(m.shape, BF16), jax.ShapeDtypeStruct(z.shape, BF16)),
            in_specs=[hbm, hbm],
            out_specs=(hbm, hbm),
            scratch_shapes=[V(m.shape, BF16), V(z.shape, BF16), S((2, E8)), S((2, E8))],
            name='finish',
        )(*outs)

    return jax.shard_map(block, mesh=mesh, in_specs=in_specs, out_specs=(rows_spec, rows_spec), check_vma=False)
```
